128 devices in a mesh: row: 8 (over x, y_hi), col: 16 (over y_lo, z, core).
Axes of the slice: x: 4, y: 4 (y_hi: 2, y_lo: 2; y = y_hi * 2 + y_lo), z: 4, core: 2. Of those that a mesh axis runs over, the one named last changes fastest.
Arguments:
- frame: bfloat16 [256, 512, 256], P('row', 'col'), may hold values from -6 to 6
- gain_attn: float32 [2, 256], replicated, may hold values from 0.1 to 1.9
- w_qkv: bfloat16 [2, 256, 768], replicated, may hold values from -2 to 2
- w_out: bfloat16 [2, 256, 256], replicated, may hold values from -1 to 1
- gain_mlp: float32 [2, 256], replicated, may hold values from 0.1 to 1.9
- w_up: bfloat16 [2, 256, 1024], replicated, may hold values from -0.375 to 0.375
- w_down: bfloat16 [2, 1024, 256], replicated, may hold values from -0.1875 to 0.1875
Outputs:
- result: bfloat16 [256, 512, 256], P('row', 'col')
The draws below stay inside these ranges and needn't reach their ends.
All inputs are finite; a program needn't handle non-finite values.
Results may differ from the reference program's by a relative error of at most 0.014.
The reference program's roundings to bfloat16 on the way count: a program that leaves them out, or rounds other values in their place, can miss the bound.
Values may be sent and summed in bfloat16 or wider, within the bound.
No kernel may reach another device: no remote copies, remote signals or barrier semaphores. Data moves between devices by JAX's collectives and lax.ppermute only.
A program may use at most 128 MiB of HBM per device.

```python
import jax
import jax.numpy as jnp
from jax import lax

D = 256
HEADS = 8
FF = 1024
SW = 8
LAYERS = 2
HI = 256
WI = 512


def draw_w_qkv(key, part):
    base = jax.random.fold_in(key, 11)
    key_q, key_k, key_v = jax.random.split(base, 3)
    head_dim = D // HEADS
    shape = (LAYERS, D, HEADS, head_dim)
    query = jax.random.normal(key_q, shape, jnp.float32) * 1.6 * D ** (-0.5)
    keys = jax.random.normal(key_k, shape, jnp.float32) * 1.6 * D ** (-0.5)
    values = jax.random.normal(key_v, shape, jnp.float32) * D ** (-0.5)
    whole = jnp.concatenate([query.reshape(LAYERS, D, D), keys.reshape(LAYERS, D, D), values.reshape(LAYERS, D, D)], axis=-1)
    return jnp.clip(whole, -2.0, 2.0).astype(jnp.bfloat16)


def level_of(stream_key, dims, shards, smallest, largest):
    factor_of = 1.0
    for dim, shards_of in shards:
        draws = jax.random.uniform(jax.random.fold_in(jax.random.fold_in(stream_key, 6), dim), (shards_of,), jnp.float32, smallest / len(shards), largest / len(shards))
        factor_of = factor_of * jnp.repeat(jnp.exp(draws), dims[dim] // shards_of).reshape((-1,) + (1,) * (len(dims) - 1 - dim))
    return factor_of


def gaussian(stream_key, dims, scale, reach, cuts=(), held_as=jnp.bfloat16):
    level = level_of(stream_key, dims, cuts, -0.22, 0.18) if cuts else 1.0
    values = jax.random.normal(stream_key, dims, jnp.float32) * scale * level
    return jnp.minimum(jnp.maximum(values, -reach), reach).astype(held_as)


def setup_inputs(seed: int = 0) -> dict:
    arg_keys = jax.random.split(jax.random.key(seed), 8)
    return {
        "frame": gaussian(arg_keys[0], (HI, WI, D), 1.0, 6.0, ((0, 8), (1, 16))),
        "gain_attn": jnp.clip(1.0 + 0.18 * jax.random.normal(arg_keys[1], (LAYERS, D), jnp.float32), 0.1, 1.9),
        "w_qkv": draw_w_qkv(jax.random.fold_in(arg_keys[7], 71), 0),
        "w_out": gaussian(arg_keys[3], (LAYERS, D, D), (D // 8) ** -0.5, 1.0),
        "gain_mlp": jnp.clip(1.0 + 0.18 * jax.random.normal(arg_keys[4], (LAYERS, D), jnp.float32), 0.1, 1.9),
        "w_up": gaussian(arg_keys[5], (LAYERS, D, FF), D ** -0.5, 0.375),
        "w_down": gaussian(arg_keys[6], (LAYERS, FF, D), FF ** -0.5, 0.1875),
    }


EPS = 1e-05

def normalize(values, gain):
    floats = values.astype(jnp.float32)
    center = floats - lax.optimization_barrier(jnp.mean(floats, axis=-1, keepdims=True))
    spread = lax.optimization_barrier(jnp.mean(center * center, axis=-1, keepdims=True))
    return (center * lax.rsqrt(spread + EPS) * gain).astype(jnp.bfloat16)

def fdot(left, right):
    return jnp.dot(left.astype(jnp.float32), right.astype(jnp.float32), precision=lax.Precision.HIGHEST)

def attend(query, keys, values):
    length = query.shape[0]
    block = 512 if length % 512 == 0 else length
    factor = query.shape[1] ** (-0.5)
    blocks = query.reshape(length // block, block, query.shape[1])

    def single(rows):
        scores = fdot(rows, keys.T) * factor
        top = lax.optimization_barrier(jnp.max(scores, axis=-1, keepdims=True))
        probs = jnp.exp(scores - top)
        total = lax.optimization_barrier(jnp.sum(probs, axis=-1, keepdims=True))
        weights = lax.optimization_barrier(probs.astype(jnp.bfloat16))
        return (fdot(weights, values) / total).astype(jnp.bfloat16)
    return lax.map(single, blocks).reshape(length, query.shape[1])

def stripes(query, keys, values):
    return lax.map(lambda group: attend(group[0], group[1], group[2]), (query, keys, values))

def reference(frame, gain_attn, w_qkv, w_out, gain_mlp, w_up, w_down):
    head_dim = D // HEADS
    half = HEADS // 2
    height, width = (frame.shape[0], frame.shape[1])
    state = frame
    for layer in range(LAYERS):
        normed = normalize(state, gain_attn[layer])
        qkv = fdot(normed.reshape(-1, D), w_qkv[layer]).astype(jnp.bfloat16).reshape(height, width, 3 * D)
        parts = [qkv[:, :, index * D:(index + 1) * D] for index in range(3)]

        def horizontal(array):
            piece = array[:, :, :half * head_dim].reshape(height // SW, SW, width, half, head_dim)
            return piece.transpose(0, 3, 1, 2, 4).reshape(-1, SW * width, head_dim)

        def vertical(array):
            piece = array[:, :, half * head_dim:].reshape(height, width // SW, SW, half, head_dim)
            return piece.transpose(1, 3, 0, 2, 4).reshape(-1, height * SW, head_dim)
        across = stripes(*[horizontal(array) for array in parts])
        across = across.reshape(height // SW, half, SW, width, head_dim).transpose(0, 2, 3, 1, 4)
        across = across.reshape(height, width, half * head_dim)
        down = stripes(*[vertical(array) for array in parts])
        down = down.reshape(width // SW, half, height, SW, head_dim).transpose(2, 0, 3, 1, 4)
        down = down.reshape(height, width, half * head_dim)
        heads = jnp.concatenate([across, down], axis=-1).reshape(-1, D)
        mixed = state.reshape(-1, D).astype(jnp.float32) + fdot(heads, w_out[layer])
        normed2 = normalize(mixed, gain_mlp[layer])
        hidden = jax.nn.gelu(fdot(normed2, w_up[layer]), approximate=True).astype(jnp.bfloat16)
        state = (mixed + fdot(hidden, w_down[layer])).astype(jnp.bfloat16).reshape(height, width, D)
    return state
```

```python
import jax
import jax.numpy as jnp
from jax import lax
from jax.experimental import pallas as pl
from jax.experimental.pallas import tpu as pltpu
from jax.sharding import PartitionSpec as P

D = 256
HEADS = 8
LAYERS = 2
EPS = 1e-05
HD = 32
SCALE = 32 ** -0.5 * 1.4426950408889634
BF = jnp.bfloat16
F32 = jnp.float32


def attend_item(get, n, put, kx, vx, sbuf, kb, qn):
    nk = n * 256
    ones = jnp.ones((16, 256), BF)
    def prep(s, c):
        kt = get(s, 32, 64)
        kk = jnp.concatenate([kt, kt], axis=0).astype(F32).T.astype(BF)
        kx[pl.ds(s * 256, 256), 0:64] = kk
        vx[:, pl.ds(s * 256, 256)] = jnp.concatenate([get(s, 64, 96), ones], axis=0)
        return c
    for s in range(n): prep(s, 0)
    chunks = nk // kb
    W = 256 * qn
    def qblock(i, c):
        qs = []
        for j in range(qn):
            q = get(i * qn + j, 0, 32).astype(F32) * SCALE
            hi = q.astype(BF)
            lo = (q - hi.astype(F32)).astype(BF)
            qs.append(jnp.concatenate([hi, lo], axis=0))
        qt = jnp.concatenate(qs, axis=1) if qn > 1 else qs[0]
        def scores(j, slot):
            sbuf[slot] = jnp.dot(kx[j * kb:(j + 1) * kb, 0:64], qt, preferred_element_type=F32)
        scores(0, 0)
        m = jnp.full((8, W), -jnp.inf, F32)
        o = jnp.zeros((48, W), F32)
        for j in range(chunks):
            if j + 1 < chunks: scores(j + 1, (j + 1) % 2)
            s = sbuf[j % 2]
            mb = jnp.max(s.reshape(kb // 8, 8, W), axis=0)
            mb = jnp.max(mb, axis=0, keepdims=True)
            mn = jnp.maximum(m, mb)
            alpha = jnp.exp2(m - mn)
            p = jnp.exp2(s.reshape(kb // 8, 8, W) - mn[None]).reshape(kb, W).astype(BF)
            pv = jnp.dot(vx[:, j * kb:(j + 1) * kb], p, preferred_element_type=F32)
            o = (o.reshape(6, 8, W) * alpha[None]).reshape(48, W) + pv if j else pv
            m = mn
        r = o[0:32] / o[32:33]
        for j in range(qn):
            put(i * qn + j, r[:, j * 256:(j + 1) * 256].astype(BF))
        return c
    lax.fori_loop(0, n // qn, qblock, 0)

def h_kernel(a_ref, o_ref, kx, vx, sbuf, *, kb, qn):
    n = a_ref.shape[0]
    def put(s, v): o_ref[s] = v
    attend_item(lambda s, lo, hi: a_ref[s, lo:hi, :], n, put, kx, vx, sbuf, kb, qn)

def v_kernel(a_ref, o_ref, kx, vx, sbuf, *, kb, qn):
    n = a_ref.shape[0]
    for it in range(a_ref.shape[1]):
        def put(s, v): o_ref[s, it] = v
        attend_item(lambda s, lo, hi: a_ref[s, it, lo:hi, :], n, put, kx, vx, sbuf, kb, qn)

def attn_h(a, kb=256, qn=4):
    n = a.shape[0]
    return pl.pallas_call(lambda *r: h_kernel(*r, kb=kb, qn=qn), out_shape=jax.ShapeDtypeStruct((n, 32, 256), BF),
        in_specs=[pl.BlockSpec(memory_space=pltpu.VMEM)], out_specs=pl.BlockSpec(memory_space=pltpu.VMEM),
        scratch_shapes=[pltpu.VMEM((n*256,128),BF), pltpu.VMEM((48,n*256),BF), pltpu.VMEM((2,kb,256*qn),F32)],
        cost_estimate=pl.CostEstimate(flops=4*(n*256)**2*256,transcendentals=(n*256)**2,bytes_accessed=2*n*128*256),
        name="attn_h")(a)
def attn_v(a, kb=256, qn=4):
    n = a.shape[0]
    return pl.pallas_call(lambda *r: v_kernel(*r, kb=kb, qn=qn), out_shape=jax.ShapeDtypeStruct((n, 2, 32, 256), BF),
        in_specs=[pl.BlockSpec(memory_space=pltpu.VMEM)], out_specs=pl.BlockSpec(memory_space=pltpu.VMEM),
        scratch_shapes=[pltpu.VMEM((n*256,128),BF), pltpu.VMEM((48,n*256),BF), pltpu.VMEM((2,kb,256*qn),F32)],
        cost_estimate=pl.CostEstimate(flops=8*(n*256)**2*256,transcendentals=2*(n*256)**2,bytes_accessed=4*n*128*256),
        name="attn_v")(a)


def norm(x, gain):
    center = x - jnp.mean(x, axis=-1, keepdims=True)
    spread = jnp.mean(center * center, axis=-1, keepdims=True)
    return center * lax.rsqrt(spread + EPS) * gain


def project(get, gain, wt_ref, c_ref, r_ref, nrm):
    for b in range(4):
        n = norm(get(b), gain)
        nrm[pl.ds(8 * b, 8)] = n.reshape(8, 4, 8, D)
        out = lax.dot_general(wt_ref[0:384, :], n.astype(BF), (((1,), (1,)), ((), ())), preferred_element_type=F32)
        c_ref[4 * b:4 * b + 4] = out.astype(BF).reshape(4, 96, 256)
    for cb in range(4):
        n = nrm[:, cb].reshape(256, D).astype(BF)
        out = lax.dot_general(wt_ref[384:768, :], n, (((1,), (1,)), ((), ())), preferred_element_type=F32)
        r_ref[2 * cb:2 * cb + 2] = out.astype(BF).reshape(2, 2, 96, 256)


def first_kernel(x_ref, gain_ref, wt_ref, c_ref, r_ref, nrm):
    project(lambda b: x_ref[8 * b:8 * b + 8].reshape(256, D).astype(F32), gain_ref[...], wt_ref, c_ref, r_ref, nrm)


def finish(x_ref, hc_ref, hv_ref, wo_ref, gain_ref, wu_ref, wd_ref, mix, put):
    tdot = lambda a, b: lax.dot_general(a, b, (((0,), (0,)), ((), ())), preferred_element_type=F32)
    for cb in range(4):
        h = hv_ref[4 * cb:4 * cb + 4].reshape(128, 256)
        mix[:, cb] = tdot(h, wo_ref[128:256, :]).reshape(32, 8, D)
    for b in range(4):
        h = hc_ref[4 * b:4 * b + 4].reshape(128, 256)
        mixed = tdot(h, wo_ref[0:128, :]) + mix[pl.ds(8 * b, 8)].reshape(256, D)
        mixed = mixed + x_ref[8 * b:8 * b + 8].reshape(256, D).astype(F32)
        n2 = norm(mixed, gain_ref[...]).astype(BF)
        up = jnp.dot(n2, wu_ref[...], preferred_element_type=F32)
        act = 0.5 * up * (1.0 + jnp.tanh(0.7978845608028654 * (up + 0.044715 * (up * up * up))))
        out = mixed + jnp.dot(act.astype(BF), wd_ref[...], preferred_element_type=F32)
        put(b, out.astype(BF))


def mid_kernel(x_ref, hc_ref, hv_ref, wo_ref, gm_ref, wu_ref, wd_ref, ga_ref, wt_ref, y_ref, c_ref, r_ref, mix, nrm):
    def put(b, v):
        y_ref[8 * b:8 * b + 8] = v.reshape(8, 32, D)

    finish(x_ref, hc_ref, hv_ref, wo_ref, gm_ref, wu_ref, wd_ref, mix, put)
    project(lambda b: y_ref[8 * b:8 * b + 8].reshape(256, D).astype(F32), ga_ref[...], wt_ref, c_ref, r_ref, nrm)


def last_kernel(x_ref, hc_ref, hv_ref, wo_ref, gm_ref, wu_ref, wd_ref, y_ref, mix):
    def put(b, v):
        y_ref[8 * b:8 * b + 8] = v.reshape(8, 32, D)

    finish(x_ref, hc_ref, hv_ref, wo_ref, gm_ref, wu_ref, wd_ref, mix, put)


VM = pl.BlockSpec(memory_space=pltpu.VMEM)
SENDS = (jax.ShapeDtypeStruct((16, 96, 256), BF), jax.ShapeDtypeStruct((8, 2, 96, 256), BF))
STATE = jax.ShapeDtypeStruct((32, 32, D), BF)
GRID4 = pltpu.VMEM((32, 4, 8, D), F32)


def call(kernel, name, outs, scratch, flops, *args):
    return pl.pallas_call(
        kernel, out_shape=outs, in_specs=[VM] * len(args), out_specs=jax.tree.map(lambda _: VM, outs),
        scratch_shapes=scratch, name=name,
        cost_estimate=pl.CostEstimate(flops=flops, transcendentals=0, bytes_accessed=1 << 20),
    )(*args)


def shards(frame, gain_attn, w_qkv, w_out, gain_mlp, w_up, w_down):
    wt = w_qkv.reshape(LAYERS, D, 3, HEADS, HD).transpose(0, 3, 2, 4, 1).reshape(LAYERS, 3 * D, D)
    ga = gain_attn.reshape(LAYERS, 1, D)
    gm = gain_mlp.reshape(LAYERS, 1, D)
    state = frame
    c, r = call(first_kernel, "first", SENDS, [GRID4], 4 << 30, state, ga[0], wt[0])
    for layer in range(LAYERS):
        c = lax.all_to_all(c, "col", 0, 0, tiled=True)
        r = lax.all_to_all(r, "row", 0, 0, tiled=True)
        hc = lax.all_to_all(attn_h(c), "col", 0, 0, tiled=True)
        hv = lax.all_to_all(attn_v(r), "row", 0, 0, tiled=True).reshape(16, 32, 256)
        rest = (state, hc, hv, w_out[layer], gm[layer], w_up[layer], w_down[layer])
        if layer + 1 < LAYERS:
            state, c, r = call(mid_kernel, "mid", (STATE,) + SENDS, [GRID4, GRID4], 8 << 30, *rest, ga[layer + 1], wt[layer + 1])
        else:
            state = call(last_kernel, "last", STATE, [GRID4], 4 << 30, *rest)
    return state


def solution(mesh):
    placed = (P("row", "col", None), P(), P(), P(), P(), P(), P())
    return jax.shard_map(
        shards, mesh=mesh, in_specs=placed, out_specs=P("row", "col", None), check_vma=False
    )
```

```python
import jax
import jax.numpy as jnp
from jax import lax
from jax.experimental import pallas as pl
from jax.experimental.pallas import tpu as pltpu
from jax.sharding import PartitionSpec as P

D = 256
LAYERS = 2
EPS = 1e-05
SCALE = 32 ** -0.5 * 1.4426950408889634
BF = jnp.bfloat16
F32 = jnp.float32


GAP = 90.0


def prepare(get, n, kx, vx, qx):
    nk = n * 256
    ones = jnp.ones((16, 256), BF)
    ksum = jnp.zeros((32, 256), F32)
    for s in range(n):
        kt = get(s, 32, 64)
        ksum = ksum + kt.astype(F32)
        kx[pl.ds(s * 256, 256), 0:80] = jnp.concatenate([kt, kt, ones], axis=0).T
        vx[0:32, pl.ds(s * 256, 256)] = get(s, 64, 96)
    vx[32:48, :] = jnp.ones((16, nk), BF)
    kmean = jnp.sum(ksum, axis=1, keepdims=True) * (1.0 / nk)
    far = jnp.zeros((1, 256), F32)
    for s in range(n):
        dev = get(s, 32, 64).astype(F32) - kmean
        far = jnp.maximum(far, jnp.sum(dev * dev, axis=0, keepdims=True))
    radius = jnp.sqrt(jnp.max(far, axis=1, keepdims=True))
    reach = jnp.zeros((1, 256), F32)
    low = jnp.zeros((15, 256), F32)
    for s in range(n):
        q = get(s, 0, 32).astype(F32) * SCALE
        hi = q.astype(BF)
        lo = (q - hi.astype(F32)).astype(BF)
        size = jnp.sqrt(jnp.sum(q * q, axis=0, keepdims=True)) * radius
        reach = jnp.maximum(reach, size)
        shift = jnp.sum(q * kmean, axis=0, keepdims=True) + size
        qx[:, pl.ds(s * 256, 256)] = jnp.concatenate([hi, lo, jnp.concatenate([-shift, low], axis=0).astype(BF)], axis=0)
    return jnp.max(reach)


def bounded(jobs, kb, qn, depth):
    W = 256 * qn
    seq = []
    for kx, vx, qt, put in jobs:
        steps = kx.shape[0] // kb
        for j in range(steps):
            seq.append((kx, vx, qt, put, j, j + 1 == steps))

    def dots(t):
        kx, _, qt, _, j, _ = seq[t]
        return jnp.dot(kx[j * kb:(j + 1) * kb, 0:80], qt(), preferred_element_type=F32)

    ahead = {t: dots(t) for t in range(depth)}
    for t, (kx, vx, qt, put, j, last) in enumerate(seq):
        if t + depth < len(seq):
            ahead[t + depth] = dots(t + depth)
        p = jnp.exp2(ahead.pop(t))
        part = jnp.sum(p.reshape(kb // 8, 8, W), axis=0)
        out = jnp.dot(vx[0:32, j * kb:(j + 1) * kb], p.astype(BF), preferred_element_type=F32)
        l, o = (part, out) if j == 0 else (l + part, o + out)
        if last:
            put((o / jnp.sum(l, axis=0, keepdims=True)).astype(BF))


def general(n, put, kx, vx, qx):
    def qblock(i, c):
        qt = qx[0:64, pl.ds(pl.multiple_of(i * 256, 256), 256)]

        def step(j, carry):
            m, o = carry
            k0 = pl.multiple_of(j * 256, 256)
            s = jnp.dot(kx[pl.ds(k0, 256), 0:64], qt, preferred_element_type=F32)
            mn = jnp.maximum(m, jnp.max(s, axis=0, keepdims=True))
            p = jnp.exp2(s - mn).astype(BF)
            return mn, o * jnp.exp2(m - mn) + jnp.dot(vx[:, pl.ds(k0, 256)], p, preferred_element_type=F32)

        _, o = lax.fori_loop(0, n, step, (jnp.full((1, 256), -jnp.inf, F32), jnp.zeros((48, 256), F32)))
        put(i, (o[0:32] / o[32:33]).astype(BF))
        return c

    lax.fori_loop(0, n, qblock, 0)


def attention(a, kb, qn, depth, group):
    items = a.shape[1] if a.ndim == 4 else 1
    n = a.shape[0]

    def kernel(a_ref, o_ref, *sc):
        refs = [sc[3 * i:3 * i + 3] for i in range(items)]

        def put(it, s, v):
            if a.ndim == 4:
                o_ref[s, it] = v
            else:
                o_ref[s] = v

        def getter(it):
            return lambda s, lo, hi: a_ref[s, it, lo:hi, :] if a.ndim == 4 else a_ref[s, lo:hi, :]

        reach = prepare(getter(0), n, *refs[0])
        for it in range(1, items):
            reach = jnp.maximum(reach, prepare(getter(it), n, *refs[it]))
        fits = reach <= GAP
        W = 256 * qn

        @pl.when(fits)
        def _():
            def body(g, c):
                jobs = []
                for it in range(items):
                    kx, vx, qx = refs[it]
                    for u in range(group):
                        i = g * group + u

                        def qt(i=i, qx=qx):
                            start = i * W if isinstance(i, int) else pl.multiple_of(i * W, W)
                            return qx[:, pl.ds(start, W)]

                        def store(r, i=i, it=it):
                            for v in range(qn):
                                put(it, i * qn + v, r[:, v * 256:(v + 1) * 256])

                        jobs.append((kx, vx, qt, store))
                bounded(jobs, kb, qn, depth)
                return c

            trips = n // (qn * group)
            if trips == 1:
                body(0, 0)
            else:
                lax.fori_loop(0, trips, body, 0)

        @pl.when(jnp.logical_not(fits))
        def _():
            for it in range(items):
                general(n, lambda s, v, it=it: put(it, s, v), *refs[it])

    vm = pl.BlockSpec(memory_space=pltpu.VMEM)
    return pl.pallas_call(
        kernel, out_shape=jax.ShapeDtypeStruct(a.shape[:-2] + (32, 256), BF), in_specs=[vm], out_specs=vm,
        scratch_shapes=[pltpu.VMEM((n * 256, 128), BF), pltpu.VMEM((48, n * 256), BF), pltpu.VMEM((80, n * 256), BF)] * items,
        compiler_params=pltpu.CompilerParams(vmem_limit_bytes=16 << 20),
        cost_estimate=pl.CostEstimate(flops=8 * items * (n * 256) ** 2 * 256, transcendentals=0, bytes_accessed=1 << 20),
        name="attn_v" if items > 1 else "attn_h",
    )(a)


def norm(x, gain):
    center = x - jnp.mean(x, axis=-1, keepdims=True)
    spread = jnp.mean(center * center, axis=-1, keepdims=True)
    return center * lax.rsqrt(spread + EPS) * gain


def tdot(a, b):
    return lax.dot_general(a, b, (((0,), (1,)), ((), ())), preferred_element_type=F32)


def project_across(get, gain, w_ref, c_ref):
    for b in range(4):
        n = norm(get(b), gain).astype(BF)
        for t in range(3):
            out = tdot(w_ref[:, t * 256:t * 256 + 128], n).astype(BF)
            c_ref[4 * b:4 * b + 4, t * 32:t * 32 + 32, :] = out.reshape(4, 32, 256)


def down_kernel(layer, x_ref, gain_ref, w_ref, r_ref):
    for cb in range(4):
        x = x_ref[:, 8 * cb:8 * cb + 8, :].astype(F32).reshape(256, D)
        n = norm(x, gain_ref[layer:layer + 1]).astype(BF)
        for t in range(3):
            out = tdot(w_ref[:, t * 256 + 128:t * 256 + 256], n).astype(BF)
            r_ref[2 * cb:2 * cb + 2, :, t * 32:t * 32 + 32, :] = out.reshape(2, 2, 32, 256)


def mix_kernel(x_ref, hc_ref, wo_ref, m_ref):
    for b in range(4):
        h = hc_ref[4 * b:4 * b + 4].reshape(128, 256)
        out = lax.dot_general(h, wo_ref[0:128, :], (((0,), (0,)), ((), ())), preferred_element_type=F32)
        m_ref[8 * b:8 * b + 8] = out.reshape(8, 32, D) + x_ref[8 * b:8 * b + 8].astype(F32)


def finish(layer, m_ref, hv_ref, wo_ref, gain_ref, wu_ref, wd_ref, mix, put):
    for cb in range(4):
        h = hv_ref[4 * cb:4 * cb + 4].reshape(128, 256)
        out = lax.dot_general(h, wo_ref[128:256, :], (((0,), (0,)), ((), ())), preferred_element_type=F32)
        mix[:, 8 * cb:8 * cb + 8, :] = out.reshape(32, 8, D)
    for b in range(4):
        mixed = (m_ref[8 * b:8 * b + 8] + mix[8 * b:8 * b + 8]).reshape(256, D)
        n2 = norm(mixed, gain_ref[layer:layer + 1]).astype(BF)
        up = jnp.dot(n2, wu_ref[...], preferred_element_type=F32)
        act = 0.5 * up * (1.0 + jnp.tanh(0.7978845608028654 * (up + 0.044715 * (up * up * up))))
        out = mixed + jnp.dot(act.astype(BF), wd_ref[...], preferred_element_type=F32)
        put(b, out.astype(BF))


def mid_kernel(layer, m_ref, hv_ref, wo_ref, gm_ref, wu_ref, wd_ref, ga_ref, w_ref, y_ref, c_ref, mix):
    def put(b, v):
        y_ref[8 * b:8 * b + 8] = v.reshape(8, 32, D)

    finish(layer, m_ref, hv_ref, wo_ref, gm_ref, wu_ref, wd_ref, mix, put)
    project_across(lambda b: y_ref[8 * b:8 * b + 8].reshape(256, D).astype(F32), ga_ref[layer + 1:layer + 2], w_ref, c_ref)


def last_kernel(layer, m_ref, hv_ref, wo_ref, gm_ref, wu_ref, wd_ref, y_ref, mix):
    def put(b, v):
        y_ref[8 * b:8 * b + 8] = v.reshape(8, 32, D)

    finish(layer, m_ref, hv_ref, wo_ref, gm_ref, wu_ref, wd_ref, mix, put)


VM = pl.BlockSpec(memory_space=pltpu.VMEM)
ACROSS = jax.ShapeDtypeStruct((16, 96, 256), BF)
DOWN = jax.ShapeDtypeStruct((8, 2, 96, 256), BF)
STATE = jax.ShapeDtypeStruct((32, 32, D), BF)
MIXED = jax.ShapeDtypeStruct((32, 32, D), F32)


def call(kernel, outs, scratch, flops, *args):
    def body(*refs):
        picked = [r.at[a[1]] if isinstance(a, tuple) else r for r, a in zip(refs, args)]
        kernel(*picked, *refs[len(args):])

    return pl.pallas_call(
        body, out_shape=outs, in_specs=[VM] * len(args), out_specs=jax.tree.map(lambda _: VM, outs),
        scratch_shapes=scratch, compiler_params=pltpu.CompilerParams(vmem_limit_bytes=24 << 20),
        cost_estimate=pl.CostEstimate(flops=flops, transcendentals=0, bytes_accessed=1 << 20),
    )(*[a[0] if isinstance(a, tuple) else a for a in args])


def shards(frame, gain_attn, w_qkv, w_out, gain_mlp, w_up, w_down):
    bind = lambda f, layer: (lambda *refs: f(layer, *refs))
    scratch = [pltpu.VMEM((32, 32, D), F32)]
    state = frame
    first = lambda x_ref, g_ref, w_ref, c_ref: project_across(
        lambda b: x_ref[8 * b:8 * b + 8].reshape(256, D).astype(F32), g_ref[0:1], w_ref, c_ref)
    c = call(first, ACROSS, [], 2 << 30, state, gain_attn, (w_qkv, 0))
    for layer in range(LAYERS):
        c = lax.all_to_all(c, "col", 0, 0, tiled=True)
        r = call(bind(down_kernel, layer), DOWN, [], 2 << 30, state, gain_attn, (w_qkv, layer))
        r = lax.all_to_all(r, "row", 0, 0, tiled=True)
        hc = attention(c, 256, 2, 2, 2)
        hc = lax.all_to_all(hc, "col", 0, 0, tiled=True)
        hv = attention(r, 256, 2, 2, 2)
        hv = lax.all_to_all(hv, "row", 0, 0, tiled=True).reshape(16, 32, 256)
        m = call(mix_kernel, MIXED, [], 1 << 30, state, hc, (w_out, layer))
        rest = (m, hv, (w_out, layer), gain_mlp, (w_up, layer), (w_down, layer))
        if layer + 1 < LAYERS:
            state, c = call(bind(mid_kernel, layer), (STATE, ACROSS), scratch, 6 << 30, *rest, gain_attn, (w_qkv, layer + 1))
        else:
            state = call(bind(last_kernel, layer), STATE, scratch, 4 << 30, *rest)
    return state


def solution(mesh):
    placed = (P("row", "col", None), P(), P(), P(), P(), P(), P())
    return jax.shard_map(
        shards, mesh=mesh, in_specs=placed, out_specs=P("row", "col", None), check_vma=False
    )
```

```python
import jax
import jax.numpy as jnp
from jax import lax
from jax.experimental import pallas as pl
from jax.experimental.pallas import tpu as pltpu
from jax.sharding import Mesh
from jax.sharding import PartitionSpec as P

D = 256
LAYERS = 2
EPS = 1e-05
SCALE = 32 ** -0.5 * 1.4426950408889634
BF = jnp.bfloat16
F32 = jnp.float32
ROW = ("x", "yh")
COL = "col"


GAP = 90.0


def prepare(get, n, kx, vx, qx):
    nk = n * 256
    ones = jnp.ones((16, 256), BF)
    ksum = jnp.zeros((32, 256), F32)
    for s in range(n):
        kt = get(s, 32, 64)
        ksum = ksum + kt.astype(F32)
        kx[pl.ds(s * 256, 256), 0:80] = jnp.concatenate([kt, kt, ones], axis=0).T
        vx[0:32, pl.ds(s * 256, 256)] = get(s, 64, 96)
    vx[32:48, :] = jnp.ones((16, nk), BF)
    kmean = jnp.sum(ksum, axis=1, keepdims=True) * (1.0 / nk)
    far = jnp.zeros((1, 256), F32)
    for s in range(n):
        dev = get(s, 32, 64).astype(F32) - kmean
        far = jnp.maximum(far, jnp.sum(dev * dev, axis=0, keepdims=True))
    radius = jnp.sqrt(jnp.max(far, axis=1, keepdims=True))
    reach = jnp.zeros((1, 256), F32)
    low = jnp.zeros((15, 256), F32)
    for s in range(n):
        q = get(s, 0, 32).astype(F32) * SCALE
        hi = q.astype(BF)
        lo = (q - hi.astype(F32)).astype(BF)
        size = jnp.sqrt(jnp.sum(q * q, axis=0, keepdims=True)) * radius
        reach = jnp.maximum(reach, size)
        shift = jnp.sum(q * kmean, axis=0, keepdims=True) + size
        qx[:, pl.ds(s * 256, 256)] = jnp.concatenate([hi, lo, jnp.concatenate([-shift, low], axis=0).astype(BF)], axis=0)
    return jnp.max(reach)


def bounded(jobs, kb, qn, depth):
    W = 256 * qn
    seq = []
    for kx, vx, qt, put in jobs:
        steps = kx.shape[0] // kb
        for j in range(steps):
            seq.append((kx, vx, qt, put, j, j + 1 == steps))

    def dots(t):
        kx, _, qt, _, j, _ = seq[t]
        return jnp.dot(kx[j * kb:(j + 1) * kb, 0:80], qt(), preferred_element_type=F32)

    ahead = {t: dots(t) for t in range(depth)}
    for t, (kx, vx, qt, put, j, last) in enumerate(seq):
        if t + depth < len(seq):
            ahead[t + depth] = dots(t + depth)
        p = jnp.exp2(ahead.pop(t))
        part = jnp.sum(p.reshape(kb // 8, 8, W), axis=0)
        out = jnp.dot(vx[0:32, j * kb:(j + 1) * kb], p.astype(BF), preferred_element_type=F32)
        l, o = (part, out) if j == 0 else (l + part, o + out)
        if last:
            put((o / jnp.sum(l, axis=0, keepdims=True)).astype(BF))


def general(n, put, kx, vx, qx):
    def qblock(i, c):
        qt = qx[0:64, pl.ds(pl.multiple_of(i * 256, 256), 256)]

        def step(j, carry):
            m, o = carry
            k0 = pl.multiple_of(j * 256, 256)
            s = jnp.dot(kx[pl.ds(k0, 256), 0:64], qt, preferred_element_type=F32)
            mn = jnp.maximum(m, jnp.max(s, axis=0, keepdims=True))
            p = jnp.exp2(s - mn).astype(BF)
            return mn, o * jnp.exp2(m - mn) + jnp.dot(vx[:, pl.ds(k0, 256)], p, preferred_element_type=F32)

        _, o = lax.fori_loop(0, n, step, (jnp.full((1, 256), -jnp.inf, F32), jnp.zeros((48, 256), F32)))
        put(i, (o[0:32] / o[32:33]).astype(BF))
        return c

    lax.fori_loop(0, n, qblock, 0)


def attend(items, n, get, put, refs, group):
    kb, qn, depth = 256, 2, 2
    reach = prepare(lambda *k: get(0, *k), n, *refs[0])
    for it in range(1, items):
        reach = jnp.maximum(reach, prepare(lambda *k, it=it: get(it, *k), n, *refs[it]))
    fits = reach <= GAP
    W = 256 * qn
    trips = n // (qn * group)

    @pl.when(fits)
    def _():
        def body(g, c):
            jobs = []
            for it in range(items):
                kx, vx, qx = refs[it]
                for u in range(group):
                    i = g * group + u

                    def qt(i=i, qx=qx):
                        return qx[:, pl.ds(pl.multiple_of(i * W, W), W)]

                    def store(r, i=i, it=it):
                        for v in range(qn):
                            put(it, i * qn + v, r[:, v * 256:(v + 1) * 256])

                    jobs.append((kx, vx, qt, store))
            bounded(jobs, kb, qn, depth)
            return c

        lax.fori_loop(0, trips, body, 0)

    @pl.when(jnp.logical_not(fits))
    def _():
        for it in range(items):
            general(n, lambda s, v, it=it: put(it, s, v), *refs[it])


def across_kernel(a_ref, o_ref, *sc):
    def put(it, s, v):
        o_ref[s] = v

    attend(1, 16, lambda it, s, lo, hi: a_ref[s, lo:hi, :], put, [sc], 2)


def split_kernel(*refs):
    for k in range(4):
        for e in range(2):
            refs[4 + e][k] = refs[k][e]


def down_attend_kernel(pos, near, far, o_ref, *sc):
    def get(it, s, lo, hi):
        return (far if s % 2 else near)[s // 2, it, lo:hi, :]

    def put(it, s, v):
        k, e = s // 2, s % 2
        o_ref[2 * ((pos[0] - k + 4) % 4) + (pos[1] + e) % 2, it] = v

    attend(2, 8, get, put, [sc[0:3], sc[3:6]], 2)


def norm(x, gain):
    center = x - jnp.mean(x, axis=-1, keepdims=True)
    spread = jnp.mean(center * center, axis=-1, keepdims=True)
    return center * lax.rsqrt(spread + EPS) * gain


def tdot(a, b):
    return lax.dot_general(a, b, (((0,), (1,)), ((), ())), preferred_element_type=F32)


def project(get, pos, gain, w_ref, c_ref, outs, nrm, all_ref):
    for b in range(4):
        n = norm(get(b), gain)
        nrm[8 * b:8 * b + 8] = n.reshape(8, 32, D)
        n = n.astype(BF)
        for t in range(3):
            out = tdot(w_ref[:, t * 256:t * 256 + 128], n).astype(BF)
            c_ref[4 * b:4 * b + 4, t * 32:t * 32 + 32, :] = out.reshape(4, 32, 256)
    for cb in range(4):
        n = nrm[:, 8 * cb:8 * cb + 8, :].reshape(256, D).astype(BF)
        k = (cb - pos[0] + 4) % 4
        for t in range(3):
            out = tdot(w_ref[:, t * 256 + 128:t * 256 + 256], n).astype(BF).reshape(2, 2, 32, 256)
            for hp in range(2):
                all_ref[k, (hp + pos[1]) % 2, :, t * 32:t * 32 + 32, :] = out[hp]
    for k in range(4):
        outs[k][...] = all_ref[k]


def first_kernel(pos, x_hbm, g_hbm, w_hbm, c_ref, s0, s1, s2, s3, nrm, all_ref, x, g, w, sems):
    copies = [pltpu.make_async_copy(g_hbm, g, sems.at[0]), pltpu.make_async_copy(w_hbm.at[0], w, sems.at[1]), pltpu.make_async_copy(x_hbm, x, sems.at[2])]
    for copy in copies:
        copy.start()
    for copy in copies:
        copy.wait()
    project(lambda b: x[8 * b:8 * b + 8].reshape(256, D).astype(F32), pos, g[0:1], w, c_ref, (s0, s1, s2, s3), nrm, all_ref)


def finish(layer, x_ref, hc_ref, hv_ref, wo_ref, gain_ref, wu_ref, wd, ready, mix, put):
    cdot = lambda h, w: lax.dot_general(h, w, (((0,), (0,)), ((), ())), preferred_element_type=F32)
    for cb in range(4):
        h = hv_ref[4 * cb:4 * cb + 4].reshape(128, 256)
        mix[:, 8 * cb:8 * cb + 8, :] = cdot(h, wo_ref[layer, 128:256, :]).reshape(32, 8, D)
    ready()
    for b in range(4):
        h = hc_ref[4 * b:4 * b + 4].reshape(128, 256)
        mixed = cdot(h, wo_ref[layer, 0:128, :]) + x_ref[8 * b:8 * b + 8].reshape(256, D).astype(F32)
        mixed = mixed + mix[8 * b:8 * b + 8].reshape(256, D)
        n2 = norm(mixed, gain_ref[layer:layer + 1]).astype(BF)
        up = jnp.dot(n2, wu_ref[layer], preferred_element_type=F32)
        act = 0.5 * up * (1.0 + jnp.tanh(0.7978845608028654 * (up + 0.044715 * (up * up * up))))
        out = mixed + jnp.dot(act.astype(BF), wd[...], preferred_element_type=F32)
        put(b, out.astype(BF))


def mid_kernel(layer, pos, x_ref, hc_ref, hv_ref, wo_ref, gm_ref, wu_ref, wd_hbm, ga_ref, w_hbm, y_hbm, c_ref, s0, s1, s2, s3, mix, all_ref, wd, y, sems, w):
    loads = [pltpu.make_async_copy(wd_hbm.at[layer], wd, sems.at[0]), pltpu.make_async_copy(w_hbm.at[layer + 1], w, sems.at[1])]
    save = pltpu.make_async_copy(y, y_hbm, sems.at[2])
    for copy in loads:
        copy.start()

    def ready():
        for copy in loads:
            copy.wait()

    def put(b, v):
        y[8 * b:8 * b + 8] = v.reshape(8, 32, D)

    finish(layer, x_ref, hc_ref, hv_ref, wo_ref, gm_ref, wu_ref, wd, ready, mix, put)
    save.start()
    project(lambda b: y[8 * b:8 * b + 8].reshape(256, D).astype(F32), pos, ga_ref[layer + 1:layer + 2], w, c_ref, (s0, s1, s2, s3), mix, all_ref)
    save.wait()


def last_kernel(layer, x_ref, hc_ref, hv_ref, wo_ref, gm_ref, wu_ref, wd_hbm, y_ref, mix, wd, sems):
    load = pltpu.make_async_copy(wd_hbm.at[layer], wd, sems.at[0])
    load.start()

    def put(b, v):
        y_ref[8 * b:8 * b + 8] = v.reshape(8, 32, D)

    finish(layer, x_ref, hc_ref, hv_ref, wo_ref, gm_ref, wu_ref, wd, load.wait, mix, put)


VM = pl.BlockSpec(memory_space=pltpu.VMEM)
HB = pl.BlockSpec(memory_space=pltpu.HBM)
SM = pl.BlockSpec(memory_space=pltpu.SMEM)
ACROSS = jax.ShapeDtypeStruct((16, 96, 256), BF)
HALF = jax.ShapeDtypeStruct((4, 2, 96, 256), BF)
BLOCK = jax.ShapeDtypeStruct((2, 2, 96, 256), BF)
STATE = jax.ShapeDtypeStruct((32, 32, D), BF)
HBM_STATE = pltpu.HBM((32, 32, D), BF)
SEMS = pltpu.SemaphoreType.DMA((3,))


def call(kernel, specs, outs, out_specs, scratch, flops, limit, *args):
    return pl.pallas_call(
        kernel, out_shape=outs, in_specs=specs, out_specs=out_specs,
        scratch_shapes=scratch, compiler_params=pltpu.CompilerParams(vmem_limit_bytes=limit << 20),
        cost_estimate=pl.CostEstimate(flops=flops, transcendentals=0, bytes_accessed=1 << 20),
    )(*args)


def far_memory(x):
    return pltpu.with_memory_space_constraint(x, pltpu.HBM)


def attention_scratch(n):
    return [pltpu.VMEM((n * 256, 128), BF), pltpu.VMEM((48, n * 256), BF), pltpu.VMEM((80, n * 256), BF)]


def shards(frame, gain_attn, w_qkv, w_out, gain_mlp, w_up, w_down):
    bind = lambda f, layer: (lambda *refs: f(layer, *refs))
    vm = lambda *shape, dtype=BF: pltpu.VMEM(shape, dtype)
    pos = jnp.stack([lax.axis_index("x"), lax.axis_index("yh")]).astype(jnp.int32)
    shift = lambda value, axis, k, size: lax.ppermute(value, axis, [(i, (i + k) % size) for i in range(size)])
    state = frame
    work = [vm(32, 32, D, dtype=F32), vm(4, 2, 2, 96, 256)]
    c, *s = call(first_kernel, [SM] + [HB] * 3, (ACROSS,) + (BLOCK,) * 4, (VM,) * 5, work + [vm(32, 32, D), vm(LAYERS, D, dtype=F32), vm(D, 3 * D), SEMS], 2 << 30, 12, pos, *map(far_memory, (state, gain_attn, w_qkv)))
    for layer in range(LAYERS):
        c = lax.all_to_all(c, COL, 0, 0, tiled=True)
        r = [s[0]] + [shift(s[k], "x", k, 4) for k in (1, 2, 3)]
        near, far = call(split_kernel, [VM] * 4, (HALF,) * 2, (VM,) * 2, [], 1 << 28, 4, *r)
        far = shift(far, "yh", 1, 2)
        hc = call(across_kernel, [VM], jax.ShapeDtypeStruct((16, 32, 256), BF), VM, attention_scratch(16), 32 << 30, 16, c)
        hc = lax.all_to_all(hc, COL, 0, 0, tiled=True)
        hv = call(down_attend_kernel, [SM] + [VM] * 2, jax.ShapeDtypeStruct((8, 2, 32, 256), BF), VM, attention_scratch(8) * 2, 16 << 30, 16, pos, near, far)
        hv = lax.all_to_all(hv, ROW, 0, 0, tiled=True).reshape(16, 32, 256)
        rest = (state, hc, hv, w_out, gain_mlp, w_up, far_memory(w_down))
        specs = [VM] * 6 + [HB]
        if layer + 1 < LAYERS:
            state, c, *s = call(bind(mid_kernel, layer), [SM] + specs + [VM, HB], (HBM_STATE, ACROSS) + (BLOCK,) * 4, (HB,) + (VM,) * 5, work + [vm(4 * D, D), vm(32, 32, D), SEMS, vm(D, 3 * D)], 6 << 30, 24, pos, *rest, gain_attn, far_memory(w_qkv))
        else:
            state = call(bind(last_kernel, layer), specs, STATE, VM, work[:1] + [vm(4 * D, D), SEMS], 4 << 30, 24, *rest)
    return state


def solution(mesh):
    torus = Mesh(mesh.devices.reshape(4, 2, mesh.shape["col"]), ("x", "yh", "col"))
    placed = (P(ROW, COL, None), P(), P(), P(), P(), P(), P())
    return jax.shard_map(
        shards, mesh=torus, in_specs=placed, out_specs=P(ROW, COL, None), check_vma=False
    )
```

```python
import jax
import jax.numpy as jnp
from jax import lax
from jax.experimental import pallas as pl
from jax.experimental.pallas import tpu as pltpu
from jax.sharding import Mesh
from jax.sharding import PartitionSpec as P

D = 256
LAYERS = 2
EPS = 1e-05
SCALE = 32 ** -0.5 * 1.4426950408889634
BF = jnp.bfloat16
F32 = jnp.float32
ROW = ("x", "yh")
COL = "col"


GAP = 90.0


def prepare(get, n, kx, vx, qx):
    nk = n * 256
    ones = jnp.ones((16, 256), BF)
    ksum = jnp.zeros((32, 256), F32)
    for s in range(n):
        kt = get(s, 32, 64)
        ksum = ksum + kt.astype(F32)
        kx[pl.ds(s * 256, 256), 0:80] = jnp.concatenate([kt, kt, ones], axis=0).T
        vx[0:32, pl.ds(s * 256, 256)] = get(s, 64, 96)
    vx[32:48, :] = jnp.ones((16, nk), BF)
    kmean = jnp.sum(ksum, axis=1, keepdims=True) * (1.0 / nk)
    far = jnp.zeros((1, 256), F32)
    for s in range(n):
        dev = get(s, 32, 64).astype(F32) - kmean
        far = jnp.maximum(far, jnp.sum(dev * dev, axis=0, keepdims=True))
    radius = jnp.sqrt(jnp.max(far, axis=1, keepdims=True))
    reach = jnp.zeros((1, 256), F32)
    low = jnp.zeros((15, 256), F32)
    for s in range(n):
        q = get(s, 0, 32).astype(F32) * SCALE
        hi = q.astype(BF)
        lo = (q - hi.astype(F32)).astype(BF)
        size = jnp.sqrt(jnp.sum(q * q, axis=0, keepdims=True)) * radius
        reach = jnp.maximum(reach, size)
        shift = jnp.sum(q * kmean, axis=0, keepdims=True) + size
        qx[:, pl.ds(s * 256, 256)] = jnp.concatenate([hi, lo, jnp.concatenate([-shift, low], axis=0).astype(BF)], axis=0)
    return jnp.max(reach)


def bounded(jobs, kb, qn, depth):
    W = 256 * qn
    seq = []
    for kx, vx, qt, put in jobs:
        steps = kx.shape[0] // kb
        for j in range(steps):
            seq.append((kx, vx, qt, put, j, j + 1 == steps))

    def dots(t):
        kx, _, qt, _, j, _ = seq[t]
        return jnp.dot(kx[j * kb:(j + 1) * kb, 0:80], qt(), preferred_element_type=F32)

    ahead = {t: dots(t) for t in range(depth)}
    for t, (kx, vx, qt, put, j, last) in enumerate(seq):
        if t + depth < len(seq):
            ahead[t + depth] = dots(t + depth)
        p = jnp.exp2(ahead.pop(t))
        part = jnp.sum(p.reshape(kb // 8, 8, W), axis=0)
        out = jnp.dot(vx[0:32, j * kb:(j + 1) * kb], p.astype(BF), preferred_element_type=F32)
        l, o = (part, out) if j == 0 else (l + part, o + out)
        if last:
            put((o / jnp.sum(l, axis=0, keepdims=True)).astype(BF))


def general(n, put, kx, vx, qx):
    def qblock(i, c):
        qt = qx[0:64, pl.ds(pl.multiple_of(i * 256, 256), 256)]

        def step(j, carry):
            m, o = carry
            k0 = pl.multiple_of(j * 256, 256)
            s = jnp.dot(kx[pl.ds(k0, 256), 0:64], qt, preferred_element_type=F32)
            mn = jnp.maximum(m, jnp.max(s, axis=0, keepdims=True))
            p = jnp.exp2(s - mn).astype(BF)
            return mn, o * jnp.exp2(m - mn) + jnp.dot(vx[:, pl.ds(k0, 256)], p, preferred_element_type=F32)

        _, o = lax.fori_loop(0, n, step, (jnp.full((1, 256), -jnp.inf, F32), jnp.zeros((48, 256), F32)))
        put(i, (o[0:32] / o[32:33]).astype(BF))
        return c

    lax.fori_loop(0, n, qblock, 0)


def attend(items, n, get, put, refs, group):
    kb, qn, depth = 256, 2, 2
    reach = prepare(lambda *k: get(0, *k), n, *refs[0])
    for it in range(1, items):
        reach = jnp.maximum(reach, prepare(lambda *k, it=it: get(it, *k), n, *refs[it]))
    fits = reach <= GAP
    W = 256 * qn
    trips = n // (qn * group)

    @pl.when(fits)
    def _():
        def body(g, c):
            jobs = []
            for it in range(items):
                kx, vx, qx = refs[it]
                for u in range(group):
                    i = g * group + u

                    def qt(i=i, qx=qx):
                        return qx[:, pl.ds(pl.multiple_of(i * W, W), W)]

                    def store(r, i=i, it=it):
                        for v in range(qn):
                            put(it, i * qn + v, r[:, v * 256:(v + 1) * 256])

                    jobs.append((kx, vx, qt, store))
            bounded(jobs, kb, qn, depth)
            return c

        lax.fori_loop(0, trips, body, 0)

    @pl.when(jnp.logical_not(fits))
    def _():
        for it in range(items):
            general(n, lambda s, v, it=it: put(it, s, v), *refs[it])


def across_kernel(a_ref, o_ref, *sc):
    def put(it, s, v):
        o_ref[s] = v

    attend(1, 16, lambda it, s, lo, hi: a_ref[s, lo:hi, :], put, [sc], 2)


def pair_kernel(near, far, *outs):
    for k in range(4):
        outs[k][0] = near[k]
        outs[k][1] = far[k]


def down_attend_kernel(p0, p1, p2, p3, near, far, all_ref, *sc):
    blocks = (p0, p1, p2, p3)

    def put(it, s, v):
        all_ref[s, it] = v

    attend(2, 8, lambda it, s, lo, hi: blocks[s // 2][s % 2, it, lo:hi, :], put, [sc[0:3], sc[3:6]], 2)
    for k in range(4):
        near[k] = all_ref[2 * k]
        far[k] = all_ref[2 * k + 1]


def norm(x, gain):
    center = x - jnp.mean(x, axis=-1, keepdims=True)
    spread = jnp.mean(center * center, axis=-1, keepdims=True)
    return center * lax.rsqrt(spread + EPS) * gain


def tdot(a, b):
    return lax.dot_general(a, b, (((0,), (1,)), ((), ())), preferred_element_type=F32)


def project(get, pos, gain, w_ref, c_ref, sends, nrm, sent):
    for b in range(4):
        n = norm(get(b), gain)
        nrm[8 * b:8 * b + 8] = n.reshape(8, 32, D)
        n = n.astype(BF)
        for t in range(3):
            out = tdot(w_ref[:, t * 256:t * 256 + 128], n).astype(BF)
            c_ref[4 * b:4 * b + 4, t * 32:t * 32 + 32, :] = out.reshape(4, 32, 256)
    sent()
    for cb in range(4):
        n = nrm[:, 8 * cb:8 * cb + 8, :].reshape(256, D).astype(BF)
        k = (cb - pos[0] + 4) % 4
        for t in range(3):
            out = tdot(w_ref[:, t * 256 + 128:t * 256 + 256], n).astype(BF).reshape(2, 2, 32, 256)
            for hp in range(2):
                sends[(hp + pos[1]) % 2, k, :, t * 32:t * 32 + 32, :] = out[hp]


def first_kernel(pos, x_hbm, g_hbm, w_hbm, c_hbm, near, far, nrm, sends, x, g, w, sems, c):
    copies = [pltpu.make_async_copy(g_hbm, g, sems.at[0]), pltpu.make_async_copy(w_hbm.at[0], w, sems.at[1]), pltpu.make_async_copy(x_hbm, x, sems.at[2])]
    save = pltpu.make_async_copy(c, c_hbm, sems.at[3])
    for copy in copies:
        copy.start()
    for copy in copies:
        copy.wait()
    project(lambda b: x[8 * b:8 * b + 8].reshape(256, D).astype(F32), pos, g[0:1], w, c, sends, nrm, save.start)
    near[...] = sends[0]
    far[...] = sends[1]
    save.wait()


def finish(layer, pos, x_ref, hc_ref, heads, wo_ref, gain_ref, wu_ref, wd, ready, mix, hv, n2, put):
    cdot = lambda h, w: lax.dot_general(h, w, (((0,), (0,)), ((), ())), preferred_element_type=F32)
    for k in range(4):
        at = 2 * ((pos[0] + k) % 4)
        hv[at + pos[1]] = heads[k][0]
        hv[at + 1 - pos[1]] = heads[k][1]
    for cb in range(4):
        h = hv[2 * cb:2 * cb + 2].reshape(128, 256)
        mix[:, 8 * cb:8 * cb + 8, :] = cdot(h, wo_ref[layer, 128:256, :]).reshape(32, 8, D)
    for b in range(4):
        rows = slice(8 * b, 8 * b + 8)
        h = hc_ref[4 * b:4 * b + 4].reshape(128, 256)
        mixed = cdot(h, wo_ref[layer, 0:128, :]) + x_ref[rows].reshape(256, D).astype(F32)
        mixed = mixed + mix[rows].reshape(256, D)
        mix[rows] = mixed.reshape(8, 32, D)
        n2[256 * b:256 * b + 256, :] = norm(mixed, gain_ref[layer:layer + 1]).astype(BF)
    ready()
    for b in range(4):
        up = jnp.dot(n2[256 * b:256 * b + 256, :], wu_ref[layer], preferred_element_type=F32)
        act = 0.5 * up * (1.0 + jnp.tanh(0.7978845608028654 * (up + 0.044715 * (up * up * up))))
        out = jnp.dot(act.astype(BF), wd[...], preferred_element_type=F32)
        put(b, (mix[8 * b:8 * b + 8].reshape(256, D) + out).astype(BF))


def mid_kernel(layer, pos, x_ref, hc_ref, h0, h1, h2, h3, wo_ref, gm_ref, wu_ref, wd_hbm, ga_ref, w_hbm, y_hbm, c_hbm, near, far, mix, sends, wd, hv, n2, sems, y, w, c):
    loads = [pltpu.make_async_copy(wd_hbm.at[layer], wd, sems.at[0]), pltpu.make_async_copy(w_hbm.at[layer + 1], w, sems.at[1])]
    saves = [pltpu.make_async_copy(y, y_hbm, sems.at[2]), pltpu.make_async_copy(c, c_hbm, sems.at[3])]
    for copy in loads:
        copy.start()

    def ready():
        for copy in loads:
            copy.wait()

    def put(b, v):
        y[8 * b:8 * b + 8] = v.reshape(8, 32, D)

    def sent():
        for copy in saves:
            copy.start()

    finish(layer, pos, x_ref, hc_ref, (h0, h1, h2, h3), wo_ref, gm_ref, wu_ref, wd, ready, mix, hv, n2, put)
    project(lambda b: y[8 * b:8 * b + 8].reshape(256, D).astype(F32), pos, ga_ref[layer + 1:layer + 2], w, c, sends, mix, sent)
    near[...] = sends[0]
    far[...] = sends[1]
    for copy in saves:
        copy.wait()


def last_kernel(layer, pos, x_ref, hc_ref, h0, h1, h2, h3, wo_ref, gm_ref, wu_ref, wd_hbm, y_ref, mix, wd, hv, n2, sems):
    load = pltpu.make_async_copy(wd_hbm.at[layer], wd, sems.at[0])
    load.start()

    def put(b, v):
        y_ref[8 * b:8 * b + 8] = v.reshape(8, 32, D)

    finish(layer, pos, x_ref, hc_ref, (h0, h1, h2, h3), wo_ref, gm_ref, wu_ref, wd, load.wait, mix, hv, n2, put)


VM = pl.BlockSpec(memory_space=pltpu.VMEM)
HB = pl.BlockSpec(memory_space=pltpu.HBM)
SM = pl.BlockSpec(memory_space=pltpu.SMEM)
REPLY = jax.ShapeDtypeStruct((2, 2, 32, 256), BF)
HALF_REPLY = jax.ShapeDtypeStruct((4, 2, 32, 256), BF)
HALF = jax.ShapeDtypeStruct((4, 2, 96, 256), BF)
BLOCK = jax.ShapeDtypeStruct((2, 2, 96, 256), BF)
STATE = jax.ShapeDtypeStruct((32, 32, D), BF)
HBM_ACROSS = pltpu.HBM((16, 96, 256), BF)
HBM_STATE = pltpu.HBM((32, 32, D), BF)
SEMS = pltpu.SemaphoreType.DMA((4,))


def call(kernel, specs, outs, out_specs, scratch, flops, limit, *args):
    return pl.pallas_call(
        kernel, out_shape=outs, in_specs=specs, out_specs=out_specs,
        scratch_shapes=scratch, compiler_params=pltpu.CompilerParams(vmem_limit_bytes=limit << 20),
        cost_estimate=pl.CostEstimate(flops=flops, transcendentals=0, bytes_accessed=1 << 20),
    )(*args)


def far_memory(x):
    return pltpu.with_memory_space_constraint(x, pltpu.HBM)


def attention_scratch(n):
    return [pltpu.VMEM((n * 256, 128), BF), pltpu.VMEM((48, n * 256), BF), pltpu.VMEM((80, n * 256), BF)]


def shards(frame, gain_attn, w_qkv, w_out, gain_mlp, w_up, w_down):
    bind = lambda f, layer: (lambda *refs: f(layer, *refs))
    vm = lambda *shape, dtype=BF: pltpu.VMEM(shape, dtype)
    pos = jnp.stack([lax.axis_index("x"), lax.axis_index("yh")]).astype(jnp.int32)
    shift = lambda value, axis, k, size: lax.ppermute(value, axis, [(i, (i + k) % size) for i in range(size)])
    state = frame
    sends = vm(2, 4, 2, 96, 256)
    mix = vm(32, 32, D, dtype=F32)
    mlp = [vm(4 * D, D), vm(8, 2, 32, 256), vm(4 * D, D), SEMS]
    buffers = [vm(D, 3 * D), vm(16, 96, 256)]
    c, near, far = call(first_kernel, [SM] + [HB] * 3, (HBM_ACROSS, HALF, HALF), (HB, VM, VM), [mix, sends, vm(32, 32, D), vm(LAYERS, D, dtype=F32), buffers[0], SEMS, buffers[1]], 2 << 30, 12, pos, *map(far_memory, (state, gain_attn, w_qkv)))
    for layer in range(LAYERS):
        far = shift(far, "yh", 1, 2)
        c = lax.all_to_all(c, COL, 0, 0, tiled=True)
        r = call(pair_kernel, [VM] * 2, (BLOCK,) * 4, (VM,) * 4, [], 1 << 28, 4, near, far)
        r = [r[0]] + [shift(r[k], "x", k, 4) for k in (1, 2, 3)]
        hc = call(across_kernel, [VM], jax.ShapeDtypeStruct((16, 32, 256), BF), VM, attention_scratch(16), 32 << 30, 16, c)
        near, far = call(down_attend_kernel, [VM] * 4, (HALF_REPLY,) * 2, (VM,) * 2, [vm(8, 2, 32, 256)] + attention_scratch(8) * 2, 16 << 30, 16, *r)
        far = shift(far, "yh", 1, 2)
        hc = lax.all_to_all(hc, COL, 0, 0, tiled=True)
        o = call(pair_kernel, [VM] * 2, (REPLY,) * 4, (VM,) * 4, [], 1 << 28, 4, near, far)
        o = [o[0]] + [shift(o[k], "x", 4 - k, 4) for k in (1, 2, 3)]
        rest = (pos, state, hc, *o, w_out, gain_mlp, w_up, far_memory(w_down))
        specs = [SM] + [VM] * 9 + [HB]
        if layer + 1 < LAYERS:
            state, c, near, far = call(bind(mid_kernel, layer), specs + [VM, HB], (HBM_STATE, HBM_ACROSS, HALF, HALF), (HB, HB, VM, VM), [mix, sends] + mlp + [vm(32, 32, D)] + buffers, 6 << 30, 24, *rest, gain_attn, far_memory(w_qkv))
        else:
            state = call(bind(last_kernel, layer), specs, STATE, VM, [mix] + mlp, 4 << 30, 24, *rest)
    return state


def solution(mesh):
    torus = Mesh(mesh.devices.reshape(4, 2, mesh.shape["col"]), ("x", "yh", "col"))
    placed = (P(ROW, COL, None), P(), P(), P(), P(), P(), P())
    return jax.shard_map(
        shards, mesh=torus, in_specs=placed, out_specs=P(ROW, COL, None), check_vma=False
    )
```

```python
import jax
import jax.numpy as jnp
from jax import lax
from jax.experimental import pallas as pl
from jax.experimental.pallas import tpu as pltpu
from jax.sharding import Mesh
from jax.sharding import PartitionSpec as P

D = 256
LAYERS = 2
EPS = 1e-05
SCALE = 32 ** -0.5 * 1.4426950408889634
BF = jnp.bfloat16
F32 = jnp.float32
ROW = ("x", "yh")
COL = "col"


GAP = 90.0


def prepare(get, n, kx, vx, qx):
    nk = n * 256
    ones = jnp.ones((16, 256), BF)
    ksum = jnp.zeros((32, 256), F32)
    for s in range(n):
        kt = get(s, 32, 64)
        ksum = ksum + kt.astype(F32)
        kx[pl.ds(s * 256, 256), 0:80] = jnp.concatenate([kt, kt, ones], axis=0).T
        vx[0:32, pl.ds(s * 256, 256)] = get(s, 64, 96)
    vx[32:48, :] = jnp.ones((16, nk), BF)
    kmean = jnp.sum(ksum, axis=1, keepdims=True) * (1.0 / nk)
    far = jnp.zeros((1, 256), F32)
    for s in range(n):
        dev = get(s, 32, 64).astype(F32) - kmean
        far = jnp.maximum(far, jnp.sum(dev * dev, axis=0, keepdims=True))
    radius = jnp.sqrt(jnp.max(far, axis=1, keepdims=True))
    reach = jnp.zeros((1, 256), F32)
    low = jnp.zeros((15, 256), F32)
    for s in range(n):
        q = get(s, 0, 32).astype(F32) * SCALE
        hi = q.astype(BF)
        lo = (q - hi.astype(F32)).astype(BF)
        size = jnp.sqrt(jnp.sum(q * q, axis=0, keepdims=True)) * radius
        reach = jnp.maximum(reach, size)
        shift = jnp.sum(q * kmean, axis=0, keepdims=True) + size
        qx[:, pl.ds(s * 256, 256)] = jnp.concatenate([hi, lo, jnp.concatenate([-shift, low], axis=0).astype(BF)], axis=0)
    return jnp.max(reach)


def bounded(jobs, kb, qn, depth):
    W = 256 * qn
    seq = []
    for kx, vx, qt, put in jobs:
        steps = kx.shape[0] // kb
        for j in range(steps):
            seq.append((kx, vx, qt, put, j, j + 1 == steps))

    def dots(t):
        kx, _, qt, _, j, _ = seq[t]
        return jnp.dot(kx[j * kb:(j + 1) * kb, 0:80], qt(), preferred_element_type=F32)

    ahead = {t: dots(t) for t in range(depth)}
    for t, (kx, vx, qt, put, j, last) in enumerate(seq):
        if t + depth < len(seq):
            ahead[t + depth] = dots(t + depth)
        p = jnp.exp2(ahead.pop(t))
        part = jnp.sum(p.reshape(kb // 8, 8, W), axis=0)
        out = jnp.dot(vx[0:32, j * kb:(j + 1) * kb], p.astype(BF), preferred_element_type=F32)
        l, o = (part, out) if j == 0 else (l + part, o + out)
        if last:
            put((o / jnp.sum(l, axis=0, keepdims=True)).astype(BF))


def general(n, put, kx, vx, qx):
    def qblock(i, c):
        qt = qx[0:64, pl.ds(pl.multiple_of(i * 256, 256), 256)]

        def step(j, carry):
            m, o = carry
            k0 = pl.multiple_of(j * 256, 256)
            s = jnp.dot(kx[pl.ds(k0, 256), 0:64], qt, preferred_element_type=F32)
            mn = jnp.maximum(m, jnp.max(s, axis=0, keepdims=True))
            p = jnp.exp2(s - mn).astype(BF)
            return mn, o * jnp.exp2(m - mn) + jnp.dot(vx[:, pl.ds(k0, 256)], p, preferred_element_type=F32)

        _, o = lax.fori_loop(0, n, step, (jnp.full((1, 256), -jnp.inf, F32), jnp.zeros((48, 256), F32)))
        put(i, (o[0:32] / o[32:33]).astype(BF))
        return c

    lax.fori_loop(0, n, qblock, 0)


def attend(items, n, get, put, refs, group):
    kb, qn, depth = 256, 2, 2
    reach = prepare(lambda *k: get(0, *k), n, *refs[0])
    for it in range(1, items):
        reach = jnp.maximum(reach, prepare(lambda *k, it=it: get(it, *k), n, *refs[it]))
    fits = reach <= GAP
    W = 256 * qn
    trips = n // (qn * group)

    @pl.when(fits)
    def _():
        def body(g, c):
            jobs = []
            for it in range(items):
                kx, vx, qx = refs[it]
                for u in range(group):
                    i = g * group + u

                    def qt(i=i, qx=qx):
                        return qx[:, pl.ds(pl.multiple_of(i * W, W), W)]

                    def store(r, i=i, it=it):
                        for v in range(qn):
                            put(it, i * qn + v, r[:, v * 256:(v + 1) * 256])

                    jobs.append((kx, vx, qt, store))
            bounded(jobs, kb, qn, depth)
            return c

        lax.fori_loop(0, trips, body, 0)

    @pl.when(jnp.logical_not(fits))
    def _():
        for it in range(items):
            general(n, lambda s, v, it=it: put(it, s, v), *refs[it])


def across_kernel(a_ref, o_ref, *sc):
    def put(it, s, v):
        o_ref[s] = v

    attend(1, 16, lambda it, s, lo, hi: a_ref[s, lo:hi, :], put, [sc], 2)


def split_kernel(*refs):
    for k in range(4):
        for e in range(2):
            refs[4 + e][k] = refs[k][e]


def pair_kernel(near, far, *outs):
    for k in range(4):
        outs[k][0] = near[k]
        outs[k][1] = far[k]


def down_attend_kernel(got_near, got_far, near, far, all_ref, *sc):
    def put(it, s, v):
        all_ref[s, it] = v

    attend(2, 8, lambda it, s, lo, hi: (got_far if s % 2 else got_near)[s // 2, it, lo:hi, :], put, [sc[0:3], sc[3:6]], 2)
    for k in range(4):
        near[k] = all_ref[2 * k]
        far[k] = all_ref[2 * k + 1]


def norm(x, gain):
    center = x - jnp.mean(x, axis=-1, keepdims=True)
    spread = jnp.mean(center * center, axis=-1, keepdims=True)
    return center * lax.rsqrt(spread + EPS) * gain


def tdot(a, b):
    return lax.dot_general(a, b, (((0,), (1,)), ((), ())), preferred_element_type=F32)


def project(get, pos, gain, w_ref, c_ref, sends, nrm, sent):
    for b in range(4):
        n = norm(get(b), gain)
        nrm[8 * b:8 * b + 8] = n.reshape(8, 32, D)
        n = n.astype(BF)
        for t in range(3):
            out = tdot(w_ref[:, t * 256:t * 256 + 128], n).astype(BF)
            c_ref[4 * b:4 * b + 4, t * 32:t * 32 + 32, :] = out.reshape(4, 32, 256)
    sent()
    for cb in range(4):
        n = nrm[:, 8 * cb:8 * cb + 8, :].reshape(256, D).astype(BF)
        k = (cb - pos[0] + 4) % 4
        for t in range(3):
            out = tdot(w_ref[:, t * 256 + 128:t * 256 + 256], n).astype(BF).reshape(2, 2, 32, 256)
            for hp in range(2):
                sends[k, (hp + pos[1]) % 2, :, t * 32:t * 32 + 32, :] = out[hp]


def first_kernel(pos, x_hbm, g_hbm, w_hbm, c_hbm, s0, s1, s2, s3, nrm, sends, x, g, w, sems, c):
    outs = (s0, s1, s2, s3)
    copies = [pltpu.make_async_copy(g_hbm, g, sems.at[0]), pltpu.make_async_copy(w_hbm.at[0], w, sems.at[1]), pltpu.make_async_copy(x_hbm, x, sems.at[2])]
    save = pltpu.make_async_copy(c, c_hbm, sems.at[3])
    for copy in copies:
        copy.start()
    for copy in copies:
        copy.wait()
    project(lambda b: x[8 * b:8 * b + 8].reshape(256, D).astype(F32), pos, g[0:1], w, c, sends, nrm, save.start)
    for k in range(4):
        outs[k][...] = sends[k]
    save.wait()


def finish(layer, pos, x_ref, hc_ref, heads, wo_ref, gain_ref, wu_ref, wd, ready, mix, hv, n2, put):
    cdot = lambda h, w: lax.dot_general(h, w, (((0,), (0,)), ((), ())), preferred_element_type=F32)
    for k in range(4):
        at = 2 * ((pos[0] + k) % 4)
        hv[at + pos[1]] = heads[k][0]
        hv[at + 1 - pos[1]] = heads[k][1]
    for cb in range(4):
        h = hv[2 * cb:2 * cb + 2].reshape(128, 256)
        mix[:, 8 * cb:8 * cb + 8, :] = cdot(h, wo_ref[layer, 128:256, :]).reshape(32, 8, D)
    for b in range(4):
        rows = slice(8 * b, 8 * b + 8)
        h = hc_ref[4 * b:4 * b + 4].reshape(128, 256)
        mixed = cdot(h, wo_ref[layer, 0:128, :]) + x_ref[rows].reshape(256, D).astype(F32)
        mixed = mixed + mix[rows].reshape(256, D)
        mix[rows] = mixed.reshape(8, 32, D)
        n2[256 * b:256 * b + 256, :] = norm(mixed, gain_ref[layer:layer + 1]).astype(BF)
    ready()
    for b in range(4):
        up = jnp.dot(n2[256 * b:256 * b + 256, :], wu_ref[layer], preferred_element_type=F32)
        act = 0.5 * up * (1.0 + jnp.tanh(0.7978845608028654 * (up + 0.044715 * (up * up * up))))
        out = jnp.dot(act.astype(BF), wd[...], preferred_element_type=F32)
        put(b, (mix[8 * b:8 * b + 8].reshape(256, D) + out).astype(BF))


def mid_kernel(layer, pos, x_ref, hc_ref, h0, h1, h2, h3, wo_ref, gm_ref, wu_ref, wd_hbm, ga_ref, w_hbm, y_hbm, c_hbm, s0, s1, s2, s3, mix, sends, wd, hv, n2, sems, y, w, c):
    outs = (s0, s1, s2, s3)
    loads = [pltpu.make_async_copy(wd_hbm.at[layer], wd, sems.at[0]), pltpu.make_async_copy(w_hbm.at[layer + 1], w, sems.at[1])]
    saves = [pltpu.make_async_copy(y, y_hbm, sems.at[2]), pltpu.make_async_copy(c, c_hbm, sems.at[3])]
    for copy in loads:
        copy.start()

    def ready():
        for copy in loads:
            copy.wait()

    def put(b, v):
        y[8 * b:8 * b + 8] = v.reshape(8, 32, D)

    def sent():
        for copy in saves:
            copy.start()

    finish(layer, pos, x_ref, hc_ref, (h0, h1, h2, h3), wo_ref, gm_ref, wu_ref, wd, ready, mix, hv, n2, put)
    project(lambda b: y[8 * b:8 * b + 8].reshape(256, D).astype(F32), pos, ga_ref[layer + 1:layer + 2], w, c, sends, mix, sent)
    for k in range(4):
        outs[k][...] = sends[k]
    for copy in saves:
        copy.wait()


def last_kernel(layer, pos, x_ref, hc_ref, h0, h1, h2, h3, wo_ref, gm_ref, wu_ref, wd_hbm, y_ref, mix, wd, hv, n2, sems):
    load = pltpu.make_async_copy(wd_hbm.at[layer], wd, sems.at[0])
    load.start()

    def put(b, v):
        y_ref[8 * b:8 * b + 8] = v.reshape(8, 32, D)

    finish(layer, pos, x_ref, hc_ref, (h0, h1, h2, h3), wo_ref, gm_ref, wu_ref, wd, load.wait, mix, hv, n2, put)


VM = pl.BlockSpec(memory_space=pltpu.VMEM)
HB = pl.BlockSpec(memory_space=pltpu.HBM)
SM = pl.BlockSpec(memory_space=pltpu.SMEM)
REPLY = jax.ShapeDtypeStruct((2, 2, 32, 256), BF)
HALF_REPLY = jax.ShapeDtypeStruct((4, 2, 32, 256), BF)
HALF = jax.ShapeDtypeStruct((4, 2, 96, 256), BF)
BLOCK = jax.ShapeDtypeStruct((2, 2, 96, 256), BF)
STATE = jax.ShapeDtypeStruct((32, 32, D), BF)
HBM_ACROSS = pltpu.HBM((16, 96, 256), BF)
HBM_STATE = pltpu.HBM((32, 32, D), BF)
SEMS = pltpu.SemaphoreType.DMA((4,))


def call(kernel, specs, outs, out_specs, scratch, flops, limit, *args):
    return pl.pallas_call(
        kernel, out_shape=outs, in_specs=specs, out_specs=out_specs,
        scratch_shapes=scratch, compiler_params=pltpu.CompilerParams(vmem_limit_bytes=limit << 20),
        cost_estimate=pl.CostEstimate(flops=flops, transcendentals=0, bytes_accessed=1 << 20),
    )(*args)


def far_memory(x):
    return pltpu.with_memory_space_constraint(x, pltpu.HBM)


def attention_scratch(n):
    return [pltpu.VMEM((n * 256, 128), BF), pltpu.VMEM((48, n * 256), BF), pltpu.VMEM((80, n * 256), BF)]


def shards(frame, gain_attn, w_qkv, w_out, gain_mlp, w_up, w_down):
    bind = lambda f, layer: (lambda *refs: f(layer, *refs))
    vm = lambda *shape, dtype=BF: pltpu.VMEM(shape, dtype)
    pos = jnp.stack([lax.axis_index("x"), lax.axis_index("yh")]).astype(jnp.int32)
    shift = lambda value, axis, k, size: lax.ppermute(value, axis, [(i, (i + k) % size) for i in range(size)])
    state = frame
    sends = vm(4, 2, 2, 96, 256)
    mix = vm(32, 32, D, dtype=F32)
    mlp = [vm(4 * D, D), vm(8, 2, 32, 256), vm(4 * D, D), SEMS]
    buffers = [vm(D, 3 * D), vm(16, 96, 256)]
    c, *r = call(first_kernel, [SM] + [HB] * 3, (HBM_ACROSS,) + (BLOCK,) * 4, (HB,) + (VM,) * 4, [mix, sends, vm(32, 32, D), vm(LAYERS, D, dtype=F32), buffers[0], SEMS, buffers[1]], 2 << 30, 12, pos, *map(far_memory, (state, gain_attn, w_qkv)))
    for layer in range(LAYERS):
        c = lax.all_to_all(c, COL, 0, 0, tiled=True)
        r = [r[0]] + [shift(r[k], "x", k, 4) for k in (1, 2, 3)]
        near, far = call(split_kernel, [VM] * 4, (HALF,) * 2, (VM,) * 2, [], 1 << 28, 4, *r)
        far = shift(far, "yh", 1, 2)
        hc = call(across_kernel, [VM], jax.ShapeDtypeStruct((16, 32, 256), BF), VM, attention_scratch(16), 32 << 30, 16, c)
        near, far = call(down_attend_kernel, [VM] * 2, (HALF_REPLY,) * 2, (VM,) * 2, [vm(8, 2, 32, 256)] + attention_scratch(8) * 2, 16 << 30, 16, near, far)
        far = shift(far, "yh", 1, 2)
        hc = lax.all_to_all(hc, COL, 0, 0, tiled=True)
        o = call(pair_kernel, [VM] * 2, (REPLY,) * 4, (VM,) * 4, [], 1 << 28, 4, near, far)
        o = [o[0]] + [shift(o[k], "x", 4 - k, 4) for k in (1, 2, 3)]
        rest = (pos, state, hc, *o, w_out, gain_mlp, w_up, far_memory(w_down))
        specs = [SM] + [VM] * 9 + [HB]
        if layer + 1 < LAYERS:
            state, c, *r = call(bind(mid_kernel, layer), specs + [VM, HB], (HBM_STATE, HBM_ACROSS) + (BLOCK,) * 4, (HB, HB) + (VM,) * 4, [mix, sends] + mlp + [vm(32, 32, D)] + buffers, 6 << 30, 24, *rest, gain_attn, far_memory(w_qkv))
        else:
            state = call(bind(last_kernel, layer), specs, STATE, VM, [mix] + mlp, 4 << 30, 24, *rest)
    return state


def solution(mesh):
    torus = Mesh(mesh.devices.reshape(4, 2, mesh.shape["col"]), ("x", "yh", "col"))
    placed = (P(ROW, COL, None), P(), P(), P(), P(), P(), P())
    return jax.shard_map(
        shards, mesh=torus, in_specs=placed, out_specs=P(ROW, COL, None), check_vma=False
    )
```

```python
import jax
import jax.numpy as jnp
from jax import lax
from jax.experimental import pallas as pl
from jax.experimental.pallas import tpu as pltpu
from jax.sharding import Mesh
from jax.sharding import PartitionSpec as P

D = 256
LAYERS = 2
EPS = 1e-05
SCALE = 32 ** -0.5 * 1.4426950408889634
BF = jnp.bfloat16
F32 = jnp.float32
ROW = ("x", "yh")
COL = "col"


GAP = 90.0


def prepare(get, n, kx, vx, qx):
    nk = n * 256
    ones = jnp.ones((16, 256), BF)
    ksum = jnp.zeros((32, 256), F32)
    for s in range(n):
        kt = get(s, 32, 64)
        ksum = ksum + kt.astype(F32)
        kx[pl.ds(s * 256, 256), 0:80] = jnp.concatenate([kt, kt, ones], axis=0).T
        vx[0:32, pl.ds(s * 256, 256)] = get(s, 64, 96)
    vx[32:48, :] = jnp.ones((16, nk), BF)
    kmean = jnp.sum(ksum, axis=1, keepdims=True) * (1.0 / nk)
    far = jnp.zeros((1, 256), F32)
    for s in range(n):
        dev = get(s, 32, 64).astype(F32) - kmean
        far = jnp.maximum(far, jnp.sum(dev * dev, axis=0, keepdims=True))
    radius = jnp.sqrt(jnp.max(far, axis=1, keepdims=True))
    reach = jnp.zeros((1, 256), F32)
    low = jnp.zeros((15, 256), F32)
    for s in range(n):
        q = get(s, 0, 32).astype(F32) * SCALE
        hi = q.astype(BF)
        lo = (q - hi.astype(F32)).astype(BF)
        size = jnp.sqrt(jnp.sum(q * q, axis=0, keepdims=True)) * radius
        reach = jnp.maximum(reach, size)
        shift = jnp.sum(q * kmean, axis=0, keepdims=True) + size
        qx[:, pl.ds(s * 256, 256)] = jnp.concatenate([hi, lo, jnp.concatenate([-shift, low], axis=0).astype(BF)], axis=0)
    return jnp.max(reach)


def bounded(jobs, kb, qn, depth):
    W = 256 * qn
    seq = []
    for kx, vx, qt, put in jobs:
        steps = kx.shape[0] // kb
        for j in range(steps):
            seq.append((kx, vx, qt, put, j, j + 1 == steps))

    def dots(t):
        kx, _, qt, _, j, _ = seq[t]
        return jnp.dot(kx[j * kb:(j + 1) * kb, 0:80], qt(), preferred_element_type=F32)

    ahead = {t: dots(t) for t in range(depth)}
    for t, (kx, vx, qt, put, j, last) in enumerate(seq):
        if t + depth < len(seq):
            ahead[t + depth] = dots(t + depth)
        p = jnp.exp2(ahead.pop(t))
        part = jnp.sum(p.reshape(kb // 8, 8, W), axis=0)
        out = jnp.dot(vx[0:32, j * kb:(j + 1) * kb], p.astype(BF), preferred_element_type=F32)
        l, o = (part, out) if j == 0 else (l + part, o + out)
        if last:
            put((o / jnp.sum(l, axis=0, keepdims=True)).astype(BF))


def general(n, put, kx, vx, qx):
    def qblock(i, c):
        qt = qx[0:64, pl.ds(pl.multiple_of(i * 256, 256), 256)]

        def step(j, carry):
            m, o = carry
            k0 = pl.multiple_of(j * 256, 256)
            s = jnp.dot(kx[pl.ds(k0, 256), 0:64], qt, preferred_element_type=F32)
            mn = jnp.maximum(m, jnp.max(s, axis=0, keepdims=True))
            p = jnp.exp2(s - mn).astype(BF)
            return mn, o * jnp.exp2(m - mn) + jnp.dot(vx[:, pl.ds(k0, 256)], p, preferred_element_type=F32)

        _, o = lax.fori_loop(0, n, step, (jnp.full((1, 256), -jnp.inf, F32), jnp.zeros((48, 256), F32)))
        put(i, (o[0:32] / o[32:33]).astype(BF))
        return c

    lax.fori_loop(0, n, qblock, 0)


def attend(items, n, get, put, refs, group):
    kb, qn, depth = 256, 2, 2
    reach = prepare(lambda *k: get(0, *k), n, *refs[0])
    for it in range(1, items):
        reach = jnp.maximum(reach, prepare(lambda *k, it=it: get(it, *k), n, *refs[it]))
    fits = reach <= GAP
    W = 256 * qn
    trips = n // (qn * group)

    @pl.when(fits)
    def _():
        def body(g, c):
            jobs = []
            for it in range(items):
                kx, vx, qx = refs[it]
                for u in range(group):
                    i = g * group + u

                    def qt(i=i, qx=qx):
                        return qx[:, pl.ds(pl.multiple_of(i * W, W), W)]

                    def store(r, i=i, it=it):
                        for v in range(qn):
                            put(it, i * qn + v, r[:, v * 256:(v + 1) * 256])

                    jobs.append((kx, vx, qt, store))
            bounded(jobs, kb, qn, depth)
            return c

        lax.fori_loop(0, trips, body, 0)

    @pl.when(jnp.logical_not(fits))
    def _():
        for it in range(items):
            general(n, lambda s, v, it=it: put(it, s, v), *refs[it])


def across_kernel(a_ref, o_ref, *sc):
    def put(it, s, v):
        o_ref[s] = v

    attend(1, 16, lambda it, s, lo, hi: a_ref[s, lo:hi, :], put, [sc], 2)


def stack_kernel(*refs):
    for k in range(4):
        refs[4][k] = refs[k][...]


def pair_kernel(near, far, *outs):
    for k in range(4):
        outs[k][0] = near[k]
        outs[k][1] = far[k]


def down_attend_kernel(n0, n1, n2, n3, got_far, near, far, all_ref, *sc):
    got_near = (n0, n1, n2, n3)

    def get(it, s, lo, hi):
        return got_far[s // 2, it, lo:hi, :] if s % 2 else got_near[s // 2][it, lo:hi, :]

    def put(it, s, v):
        all_ref[s, it] = v

    attend(2, 8, get, put, [sc[0:3], sc[3:6]], 2)
    for k in range(4):
        near[k] = all_ref[2 * k]
        far[k] = all_ref[2 * k + 1]


def norm(x, gain):
    center = x - jnp.mean(x, axis=-1, keepdims=True)
    spread = jnp.mean(center * center, axis=-1, keepdims=True)
    return center * lax.rsqrt(spread + EPS) * gain


def tdot(a, b):
    return lax.dot_general(a, b, (((0,), (1,)), ((), ())), preferred_element_type=F32)


def project(get, pos, gain, w_ref, c_ref, sends, nrm, sent):
    for b in range(4):
        n = norm(get(b), gain)
        nrm[8 * b:8 * b + 8] = n.reshape(8, 32, D)
        n = n.astype(BF)
        for t in range(3):
            out = tdot(w_ref[:, t * 256:t * 256 + 128], n).astype(BF)
            c_ref[4 * b:4 * b + 4, t * 32:t * 32 + 32, :] = out.reshape(4, 32, 256)
    sent()
    for cb in range(4):
        n = nrm[:, 8 * cb:8 * cb + 8, :].reshape(256, D).astype(BF)
        k = (cb - pos[0] + 4) % 4
        for t in range(3):
            out = tdot(w_ref[:, t * 256 + 128:t * 256 + 256], n).astype(BF).reshape(2, 2, 32, 256)
            for hp in range(2):
                sends[k, (hp + pos[1]) % 2, :, t * 32:t * 32 + 32, :] = out[hp]


def first_kernel(pos, x_hbm, g_hbm, w_hbm, c_hbm, *rest):
    outs, (nrm, sends, x, g, w, sems, c) = rest[:8], rest[8:]
    copies = [pltpu.make_async_copy(g_hbm, g, sems.at[0]), pltpu.make_async_copy(w_hbm.at[0], w, sems.at[1]), pltpu.make_async_copy(x_hbm, x, sems.at[2])]
    save = pltpu.make_async_copy(c, c_hbm, sems.at[3])
    for copy in copies:
        copy.start()
    for copy in copies:
        copy.wait()
    project(lambda b: x[8 * b:8 * b + 8].reshape(256, D).astype(F32), pos, g[0:1], w, c, sends, nrm, save.start)
    for k in range(4):
        for e in range(2):
            outs[4 * e + k][...] = sends[k, e]
    save.wait()


def finish(layer, pos, x_ref, hc_ref, heads, wo_ref, gain_ref, wu_ref, wd, ready, mix, hv, n2, put):
    cdot = lambda h, w: lax.dot_general(h, w, (((0,), (0,)), ((), ())), preferred_element_type=F32)
    for k in range(4):
        at = 2 * ((pos[0] + k) % 4)
        hv[at + pos[1]] = heads[k][0]
        hv[at + 1 - pos[1]] = heads[k][1]
    for cb in range(4):
        h = hv[2 * cb:2 * cb + 2].reshape(128, 256)
        mix[:, 8 * cb:8 * cb + 8, :] = cdot(h, wo_ref[layer, 128:256, :]).reshape(32, 8, D)
    for b in range(4):
        rows = slice(8 * b, 8 * b + 8)
        h = hc_ref[4 * b:4 * b + 4].reshape(128, 256)
        mixed = cdot(h, wo_ref[layer, 0:128, :]) + x_ref[rows].reshape(256, D).astype(F32)
        mixed = mixed + mix[rows].reshape(256, D)
        mix[rows] = mixed.reshape(8, 32, D)
        n2[256 * b:256 * b + 256, :] = norm(mixed, gain_ref[layer:layer + 1]).astype(BF)
    ready()
    for b in range(4):
        up = jnp.dot(n2[256 * b:256 * b + 256, :], wu_ref[layer], preferred_element_type=F32)
        act = 0.5 * up * (1.0 + jnp.tanh(0.7978845608028654 * (up + 0.044715 * (up * up * up))))
        out = jnp.dot(act.astype(BF), wd[...], preferred_element_type=F32)
        put(b, (mix[8 * b:8 * b + 8].reshape(256, D) + out).astype(BF))


def mid_kernel(layer, pos, x_ref, hc_ref, h0, h1, h2, h3, wo_ref, gm_ref, wu_ref, wd_hbm, ga_ref, w_hbm, y_hbm, c_hbm, *rest):
    outs, (mix, sends, wd, hv, n2, sems, y, w, c) = rest[:8], rest[8:]
    loads = [pltpu.make_async_copy(wd_hbm.at[layer], wd, sems.at[0]), pltpu.make_async_copy(w_hbm.at[layer + 1], w, sems.at[1])]
    saves = [pltpu.make_async_copy(y, y_hbm, sems.at[2]), pltpu.make_async_copy(c, c_hbm, sems.at[3])]
    for copy in loads:
        copy.start()

    def ready():
        for copy in loads:
            copy.wait()

    def put(b, v):
        y[8 * b:8 * b + 8] = v.reshape(8, 32, D)

    def sent():
        for copy in saves:
            copy.start()

    finish(layer, pos, x_ref, hc_ref, (h0, h1, h2, h3), wo_ref, gm_ref, wu_ref, wd, ready, mix, hv, n2, put)
    project(lambda b: y[8 * b:8 * b + 8].reshape(256, D).astype(F32), pos, ga_ref[layer + 1:layer + 2], w, c, sends, mix, sent)
    for k in range(4):
        for e in range(2):
            outs[4 * e + k][...] = sends[k, e]
    for copy in saves:
        copy.wait()


def last_kernel(layer, pos, x_ref, hc_ref, h0, h1, h2, h3, wo_ref, gm_ref, wu_ref, wd_hbm, y_ref, mix, wd, hv, n2, sems):
    load = pltpu.make_async_copy(wd_hbm.at[layer], wd, sems.at[0])
    load.start()

    def put(b, v):
        y_ref[8 * b:8 * b + 8] = v.reshape(8, 32, D)

    finish(layer, pos, x_ref, hc_ref, (h0, h1, h2, h3), wo_ref, gm_ref, wu_ref, wd, load.wait, mix, hv, n2, put)


VM = pl.BlockSpec(memory_space=pltpu.VMEM)
HB = pl.BlockSpec(memory_space=pltpu.HBM)
SM = pl.BlockSpec(memory_space=pltpu.SMEM)
REPLY = jax.ShapeDtypeStruct((2, 2, 32, 256), BF)
HALF_REPLY = jax.ShapeDtypeStruct((4, 2, 32, 256), BF)
HALF = jax.ShapeDtypeStruct((4, 2, 96, 256), BF)
BLOCK = jax.ShapeDtypeStruct((2, 96, 256), BF)
STATE = jax.ShapeDtypeStruct((32, 32, D), BF)
HBM_ACROSS = pltpu.HBM((16, 96, 256), BF)
HBM_STATE = pltpu.HBM((32, 32, D), BF)
SEMS = pltpu.SemaphoreType.DMA((4,))


def call(kernel, specs, outs, out_specs, scratch, flops, limit, *args):
    return pl.pallas_call(
        kernel, out_shape=outs, in_specs=specs, out_specs=out_specs,
        scratch_shapes=scratch, compiler_params=pltpu.CompilerParams(vmem_limit_bytes=limit << 20),
        cost_estimate=pl.CostEstimate(flops=flops, transcendentals=0, bytes_accessed=1 << 20),
    )(*args)


def far_memory(x):
    return pltpu.with_memory_space_constraint(x, pltpu.HBM)


def attention_scratch(n):
    return [pltpu.VMEM((n * 256, 128), BF), pltpu.VMEM((48, n * 256), BF), pltpu.VMEM((80, n * 256), BF)]


def shards(frame, gain_attn, w_qkv, w_out, gain_mlp, w_up, w_down):
    bind = lambda f, layer: (lambda *refs: f(layer, *refs))
    vm = lambda *shape, dtype=BF: pltpu.VMEM(shape, dtype)
    pos = jnp.stack([lax.axis_index("x"), lax.axis_index("yh")]).astype(jnp.int32)
    shift = lambda value, axis, k, size: lax.ppermute(value, axis, [(i, (i + k) % size) for i in range(size)])
    state = frame
    sends = vm(4, 2, 2, 96, 256)
    mix = vm(32, 32, D, dtype=F32)
    mlp = [vm(4 * D, D), vm(8, 2, 32, 256), vm(4 * D, D), SEMS]
    buffers = [vm(D, 3 * D), vm(16, 96, 256)]
    c, *r = call(first_kernel, [SM] + [HB] * 3, (HBM_ACROSS,) + (BLOCK,) * 8, (HB,) + (VM,) * 8, [mix, sends, vm(32, 32, D), vm(LAYERS, D, dtype=F32), buffers[0], SEMS, buffers[1]], 2 << 30, 12, pos, *map(far_memory, (state, gain_attn, w_qkv)))
    for layer in range(LAYERS):
        c = lax.all_to_all(c, COL, 0, 0, tiled=True)
        far = [r[4]] + [shift(r[4 + k], "x", k, 4) for k in (1, 2, 3)]
        near = [r[0]] + [shift(r[k], "x", k, 4) for k in (1, 2, 3)]
        far = call(stack_kernel, [VM] * 4, HALF, VM, [], 1 << 28, 4, *far)
        far = shift(far, "yh", 1, 2)
        hc = call(across_kernel, [VM], jax.ShapeDtypeStruct((16, 32, 256), BF), VM, attention_scratch(16), 32 << 30, 16, c)
        near, far = call(down_attend_kernel, [VM] * 5, (HALF_REPLY,) * 2, (VM,) * 2, [vm(8, 2, 32, 256)] + attention_scratch(8) * 2, 16 << 30, 16, *near, far)
        far = shift(far, "yh", 1, 2)
        hc = lax.all_to_all(hc, COL, 0, 0, tiled=True)
        o = call(pair_kernel, [VM] * 2, (REPLY,) * 4, (VM,) * 4, [], 1 << 28, 4, near, far)
        o = [o[0]] + [shift(o[k], "x", 4 - k, 4) for k in (1, 2, 3)]
        rest = (pos, state, hc, *o, w_out, gain_mlp, w_up, far_memory(w_down))
        specs = [SM] + [VM] * 9 + [HB]
        if layer + 1 < LAYERS:
            state, c, *r = call(bind(mid_kernel, layer), specs + [VM, HB], (HBM_STATE, HBM_ACROSS) + (BLOCK,) * 8, (HB, HB) + (VM,) * 8, [mix, sends] + mlp + [vm(32, 32, D)] + buffers, 6 << 30, 24, *rest, gain_attn, far_memory(w_qkv))
        else:
            state = call(bind(last_kernel, layer), specs, STATE, VM, [mix] + mlp, 4 << 30, 24, *rest)
    return state


def solution(mesh):
    torus = Mesh(mesh.devices.reshape(4, 2, mesh.shape["col"]), ("x", "yh", "col"))
    placed = (P(ROW, COL, None), P(), P(), P(), P(), P(), P())
    return jax.shard_map(
        shards, mesh=torus, in_specs=placed, out_specs=P(ROW, COL, None), check_vma=False
    )
```

```python
import jax
import jax.numpy as jnp
from jax import lax
from jax.experimental import pallas as pl
from jax.experimental.pallas import tpu as pltpu
from jax.sharding import Mesh
from jax.sharding import PartitionSpec as P

D = 256
LAYERS = 2
EPS = 1e-05
SCALE = 32 ** -0.5 * 1.4426950408889634
BF = jnp.bfloat16
F32 = jnp.float32
ROW = ("x", "yh")
COL = "col"


GAP = 90.0


def prepare(get, n, kx, vx, qx):
    nk = n * 256
    ones = jnp.ones((16, 256), BF)
    ksum = jnp.zeros((32, 256), F32)
    for s in range(n):
        kt = get(s, 32, 64)
        ksum = ksum + kt.astype(F32)
        kx[pl.ds(s * 256, 256), 0:80] = jnp.concatenate([kt, kt, ones], axis=0).T
        vx[0:32, pl.ds(s * 256, 256)] = get(s, 64, 96)
    vx[32:48, :] = jnp.ones((16, nk), BF)
    kmean = jnp.sum(ksum, axis=1, keepdims=True) * (1.0 / nk)
    far = jnp.zeros((1, 256), F32)
    for s in range(n):
        dev = get(s, 32, 64).astype(F32) - kmean
        far = jnp.maximum(far, jnp.sum(dev * dev, axis=0, keepdims=True))
    radius = jnp.sqrt(jnp.max(far, axis=1, keepdims=True))
    reach = jnp.zeros((1, 256), F32)
    low = jnp.zeros((15, 256), F32)
    for s in range(n):
        q = get(s, 0, 32).astype(F32) * SCALE
        hi = q.astype(BF)
        lo = (q - hi.astype(F32)).astype(BF)
        size = jnp.sqrt(jnp.sum(q * q, axis=0, keepdims=True)) * radius
        reach = jnp.maximum(reach, size)
        shift = jnp.sum(q * kmean, axis=0, keepdims=True) + size
        qx[:, pl.ds(s * 256, 256)] = jnp.concatenate([hi, lo, jnp.concatenate([-shift, low], axis=0).astype(BF)], axis=0)
    return jnp.max(reach)


def bounded(jobs, kb, qn, depth):
    W = 256 * qn
    seq = []
    for kx, vx, qt, put in jobs:
        steps = kx.shape[0] // kb
        for j in range(steps):
            seq.append((kx, vx, qt, put, j, j + 1 == steps))

    def dots(t):
        kx, _, qt, _, j, _ = seq[t]
        return jnp.dot(kx[j * kb:(j + 1) * kb, 0:80], qt(), preferred_element_type=F32)

    ahead = {t: dots(t) for t in range(depth)}
    for t, (kx, vx, qt, put, j, last) in enumerate(seq):
        if t + depth < len(seq):
            ahead[t + depth] = dots(t + depth)
        p = jnp.exp2(ahead.pop(t))
        part = jnp.sum(p.reshape(kb // 8, 8, W), axis=0)
        out = jnp.dot(vx[0:32, j * kb:(j + 1) * kb], p.astype(BF), preferred_element_type=F32)
        l, o = (part, out) if j == 0 else (l + part, o + out)
        if last:
            put((o / jnp.sum(l, axis=0, keepdims=True)).astype(BF))


def general(n, put, kx, vx, qx):
    def qblock(i, c):
        qt = qx[0:64, pl.ds(pl.multiple_of(i * 256, 256), 256)]

        def step(j, carry):
            m, o = carry
            k0 = pl.multiple_of(j * 256, 256)
            s = jnp.dot(kx[pl.ds(k0, 256), 0:64], qt, preferred_element_type=F32)
            mn = jnp.maximum(m, jnp.max(s, axis=0, keepdims=True))
            p = jnp.exp2(s - mn).astype(BF)
            return mn, o * jnp.exp2(m - mn) + jnp.dot(vx[:, pl.ds(k0, 256)], p, preferred_element_type=F32)

        _, o = lax.fori_loop(0, n, step, (jnp.full((1, 256), -jnp.inf, F32), jnp.zeros((48, 256), F32)))
        put(i, (o[0:32] / o[32:33]).astype(BF))
        return c

    lax.fori_loop(0, n, qblock, 0)


def attend(items, n, get, put, refs, group):
    kb, qn, depth = 256, 2, 2
    reach = prepare(lambda *k: get(0, *k), n, *refs[0])
    for it in range(1, items):
        reach = jnp.maximum(reach, prepare(lambda *k, it=it: get(it, *k), n, *refs[it]))
    fits = reach <= GAP
    W = 256 * qn
    trips = n // (qn * group)

    @pl.when(fits)
    def _():
        def body(g, c):
            jobs = []
            for it in range(items):
                kx, vx, qx = refs[it]
                for u in range(group):
                    i = g * group + u

                    def qt(i=i, qx=qx):
                        return qx[:, pl.ds(pl.multiple_of(i * W, W), W)]

                    def store(r, i=i, it=it):
                        for v in range(qn):
                            put(it, i * qn + v, r[:, v * 256:(v + 1) * 256])

                    jobs.append((kx, vx, qt, store))
            bounded(jobs, kb, qn, depth)
            return c

        lax.fori_loop(0, trips, body, 0)

    @pl.when(jnp.logical_not(fits))
    def _():
        for it in range(items):
            general(n, lambda s, v, it=it: put(it, s, v), *refs[it])


def across_kernel(a_ref, o_ref, *sc):
    def put(it, s, v):
        o_ref[s] = v

    attend(1, 16, lambda it, s, lo, hi: a_ref[s, lo:hi, :], put, [sc], 2)


def stack_kernel(*refs):
    for k in range(4):
        refs[4][k] = refs[k][...]


def pair_kernel(near, far, *outs):
    for k in range(4):
        outs[k][0] = near[k]
        outs[k][1] = far[k]


def down_attend_kernel(n0, n1, n2, n3, got_far, near, far, all_ref, *sc):
    got_near = (n0, n1, n2, n3)

    def get(it, s, lo, hi):
        return got_far[s // 2, it, lo:hi, :] if s % 2 else got_near[s // 2][it, lo:hi, :]

    def put(it, s, v):
        all_ref[s, it] = v

    attend(2, 8, get, put, [sc[0:3], sc[3:6]], 2)
    for k in range(4):
        near[k] = all_ref[2 * k]
        far[k] = all_ref[2 * k + 1]


def norm(x, gain):
    center = x - jnp.mean(x, axis=-1, keepdims=True)
    spread = jnp.mean(center * center, axis=-1, keepdims=True)
    return center * lax.rsqrt(spread + EPS) * gain


def tdot(a, b):
    return lax.dot_general(a, b, (((0,), (1,)), ((), ())), preferred_element_type=F32)


def project(get, pos, gain, w_ref, c_ref, sends, nrm, sent):
    for b in range(4):
        n = norm(get(b), gain)
        nrm[8 * b:8 * b + 8] = n.reshape(8, 32, D)
        n = n.astype(BF)
        for t in range(3):
            out = tdot(w_ref[:, t * 256:t * 256 + 128], n).astype(BF)
            c_ref[4 * b:4 * b + 4, t * 32:t * 32 + 32, :] = out.reshape(4, 32, 256)
    sent()
    for cb in range(4):
        n = nrm[:, 8 * cb:8 * cb + 8, :].reshape(256, D).astype(BF)
        k = (cb - pos[0] + 4) % 4
        for t in range(3):
            out = tdot(w_ref[:, t * 256 + 128:t * 256 + 256], n).astype(BF).reshape(2, 2, 32, 256)
            for hp in range(2):
                sends[k, (hp + pos[1]) % 2, :, t * 32:t * 32 + 32, :] = out[hp]


def first_kernel(pos, x_hbm, g_hbm, w_hbm, c_hbm, *rest):
    outs, (nrm, sends, x, g, w, sems, c) = rest[:8], rest[8:]
    copies = [pltpu.make_async_copy(g_hbm, g, sems.at[0]), pltpu.make_async_copy(w_hbm.at[0], w, sems.at[1]), pltpu.make_async_copy(x_hbm, x, sems.at[2])]
    save = pltpu.make_async_copy(c, c_hbm, sems.at[3])
    for copy in copies:
        copy.start()
    for copy in copies:
        copy.wait()
    project(lambda b: x[8 * b:8 * b + 8].reshape(256, D).astype(F32), pos, g[0:1], w, c, sends, nrm, save.start)
    for k in range(4):
        for e in range(2):
            outs[4 * e + k][...] = sends[k, e]
    save.wait()


def finish(layer, pos, x_ref, hc_ref, heads, wo_ref, gain_ref, wu, wd, ready, mix, hv, n2, put):
    cdot = lambda h, w: lax.dot_general(h, w, (((0,), (0,)), ((), ())), preferred_element_type=F32)
    for k in range(4):
        at = 2 * ((pos[0] + k) % 4)
        hv[at + pos[1]] = heads[k][0]
        hv[at + 1 - pos[1]] = heads[k][1]
    for cb in range(4):
        h = hv[2 * cb:2 * cb + 2].reshape(128, 256)
        mix[:, 8 * cb:8 * cb + 8, :] = cdot(h, wo_ref[layer, 128:256, :]).reshape(32, 8, D)
    for b in range(4):
        rows = slice(8 * b, 8 * b + 8)
        h = hc_ref[4 * b:4 * b + 4].reshape(128, 256)
        mixed = cdot(h, wo_ref[layer, 0:128, :]) + x_ref[rows].reshape(256, D).astype(F32)
        mixed = mixed + mix[rows].reshape(256, D)
        mix[rows] = mixed.reshape(8, 32, D)
        n2[256 * b:256 * b + 256, :] = norm(mixed, gain_ref[layer:layer + 1]).astype(BF)
    ready()
    for b in range(4):
        up = jnp.dot(n2[256 * b:256 * b + 256, :], wu[...], preferred_element_type=F32)
        act = 0.5 * up * (1.0 + jnp.tanh(0.7978845608028654 * (up + 0.044715 * (up * up * up))))
        out = jnp.dot(act.astype(BF), wd[...], preferred_element_type=F32)
        put(b, (mix[8 * b:8 * b + 8].reshape(256, D) + out).astype(BF))


def mid_kernel(layer, pos, x_ref, hc_ref, h0, h1, h2, h3, wo_ref, gm_ref, wu_hbm, wd_hbm, ga_ref, w_hbm, y_hbm, c_hbm, *rest):
    outs, (mix, sends, wd, wu, hv, n2, sems, y, w, c) = rest[:8], rest[8:]
    loads = [pltpu.make_async_copy(wu_hbm.at[layer], wu, sems.at[4]), pltpu.make_async_copy(wd_hbm.at[layer], wd, sems.at[0]), pltpu.make_async_copy(w_hbm.at[layer + 1], w, sems.at[1])]
    saves = [pltpu.make_async_copy(y, y_hbm, sems.at[2]), pltpu.make_async_copy(c, c_hbm, sems.at[3])]
    for copy in loads:
        copy.start()

    def ready():
        for copy in loads:
            copy.wait()

    def put(b, v):
        y[8 * b:8 * b + 8] = v.reshape(8, 32, D)

    def sent():
        for copy in saves:
            copy.start()

    finish(layer, pos, x_ref, hc_ref, (h0, h1, h2, h3), wo_ref, gm_ref, wu, wd, ready, mix, hv, n2, put)
    project(lambda b: y[8 * b:8 * b + 8].reshape(256, D).astype(F32), pos, ga_ref[layer + 1:layer + 2], w, c, sends, mix, sent)
    for k in range(4):
        for e in range(2):
            outs[4 * e + k][...] = sends[k, e]
    for copy in saves:
        copy.wait()


def last_kernel(layer, pos, x_ref, hc_ref, h0, h1, h2, h3, wo_ref, gm_ref, wu_hbm, wd_hbm, y_ref, mix, wd, wu, hv, n2, sems):
    loads = [pltpu.make_async_copy(wu_hbm.at[layer], wu, sems.at[4]), pltpu.make_async_copy(wd_hbm.at[layer], wd, sems.at[0])]
    for copy in loads:
        copy.start()

    def ready():
        for copy in loads:
            copy.wait()

    def put(b, v):
        y_ref[8 * b:8 * b + 8] = v.reshape(8, 32, D)

    finish(layer, pos, x_ref, hc_ref, (h0, h1, h2, h3), wo_ref, gm_ref, wu, wd, ready, mix, hv, n2, put)


VM = pl.BlockSpec(memory_space=pltpu.VMEM)
HB = pl.BlockSpec(memory_space=pltpu.HBM)
SM = pl.BlockSpec(memory_space=pltpu.SMEM)
REPLY = jax.ShapeDtypeStruct((2, 2, 32, 256), BF)
HALF_REPLY = jax.ShapeDtypeStruct((4, 2, 32, 256), BF)
HALF = jax.ShapeDtypeStruct((4, 2, 96, 256), BF)
BLOCK = jax.ShapeDtypeStruct((2, 96, 256), BF)
STATE = jax.ShapeDtypeStruct((32, 32, D), BF)
HBM_ACROSS = pltpu.HBM((16, 96, 256), BF)
HBM_STATE = pltpu.HBM((32, 32, D), BF)
SEMS = pltpu.SemaphoreType.DMA((5,))


def call(kernel, specs, outs, out_specs, scratch, flops, limit, *args):
    return pl.pallas_call(
        kernel, out_shape=outs, in_specs=specs, out_specs=out_specs,
        scratch_shapes=scratch, compiler_params=pltpu.CompilerParams(vmem_limit_bytes=limit << 20),
        cost_estimate=pl.CostEstimate(flops=flops, transcendentals=0, bytes_accessed=1 << 20),
    )(*args)


def far_memory(x):
    return pltpu.with_memory_space_constraint(x, pltpu.HBM)


def attention_scratch(n):
    return [pltpu.VMEM((n * 256, 128), BF), pltpu.VMEM((48, n * 256), BF), pltpu.VMEM((80, n * 256), BF)]


def shards(frame, gain_attn, w_qkv, w_out, gain_mlp, w_up, w_down):
    bind = lambda f, layer: (lambda *refs: f(layer, *refs))
    vm = lambda *shape, dtype=BF: pltpu.VMEM(shape, dtype)
    pos = jnp.stack([lax.axis_index("x"), lax.axis_index("yh")]).astype(jnp.int32)
    shift = lambda value, axis, k, size: lax.ppermute(value, axis, [(i, (i + k) % size) for i in range(size)])
    state = frame
    sends = vm(4, 2, 2, 96, 256)
    mix = vm(32, 32, D, dtype=F32)
    mlp = [vm(4 * D, D), vm(D, 4 * D), vm(8, 2, 32, 256), vm(4 * D, D), SEMS]
    buffers = [vm(D, 3 * D), vm(16, 96, 256)]
    c, *r = call(first_kernel, [SM] + [HB] * 3, (HBM_ACROSS,) + (BLOCK,) * 8, (HB,) + (VM,) * 8, [mix, sends, vm(32, 32, D), vm(LAYERS, D, dtype=F32), buffers[0], SEMS, buffers[1]], 2 << 30, 12, pos, *map(far_memory, (state, gain_attn, w_qkv)))
    for layer in range(LAYERS):
        c = lax.all_to_all(c, COL, 0, 0, tiled=True)
        far = [r[4]] + [shift(r[4 + k], "x", k, 4) for k in (1, 2, 3)]
        near = [r[0]] + [shift(r[k], "x", k, 4) for k in (1, 2, 3)]
        far = call(stack_kernel, [VM] * 4, HALF, VM, [], 1 << 28, 4, *far)
        far = shift(far, "yh", 1, 2)
        hc = call(across_kernel, [VM], jax.ShapeDtypeStruct((16, 32, 256), BF), VM, attention_scratch(16), 32 << 30, 16, c)
        near, far = call(down_attend_kernel, [VM] * 5, (HALF_REPLY,) * 2, (VM,) * 2, [vm(8, 2, 32, 256)] + attention_scratch(8) * 2, 16 << 30, 16, *near, far)
        far = shift(far, "yh", 1, 2)
        hc = lax.all_to_all(hc, COL, 0, 0, tiled=True)
        o = call(pair_kernel, [VM] * 2, (REPLY,) * 4, (VM,) * 4, [], 1 << 28, 4, near, far)
        o = [o[0]] + [shift(o[k], "x", 4 - k, 4) for k in (1, 2, 3)]
        rest = (pos, state, hc, *o, w_out, gain_mlp, far_memory(w_up), far_memory(w_down))
        specs = [SM] + [VM] * 8 + [HB] * 2
        if layer + 1 < LAYERS:
            state, c, *r = call(bind(mid_kernel, layer), specs + [VM, HB], (HBM_STATE, HBM_ACROSS) + (BLOCK,) * 8, (HB, HB) + (VM,) * 8, [mix, sends] + mlp + [vm(32, 32, D)] + buffers, 6 << 30, 24, *rest, gain_attn, far_memory(w_qkv))
        else:
            state = call(bind(last_kernel, layer), specs, STATE, VM, [mix] + mlp, 4 << 30, 24, *rest)
    return state


def solution(mesh):
    torus = Mesh(mesh.devices.reshape(4, 2, mesh.shape["col"]), ("x", "yh", "col"))
    placed = (P(ROW, COL, None), P(), P(), P(), P(), P(), P())
    return jax.shard_map(
        shards, mesh=torus, in_specs=placed, out_specs=P(ROW, COL, None), check_vma=False
    )
```
